32 devices in a mesh: dp: 4 (over z), row: 2 (over x), col: 4 (over y, core).
Axes of the slice: x: 2, y: 2, z: 4, core: 2. Of those that a mesh axis runs over, the one named last changes fastest.
Arguments:
- grad: bfloat16 [4, 4096, 14336], P('dp', 'row', 'col'), may hold values from -6 to 6
- error: bfloat16 [4, 4096, 14336], P('dp', 'row', 'col'), may hold values from -6 to 6
- q_init: float32 [14336, 128], P('col'), may hold values from -6 to 6
Outputs:
- new_error: bfloat16 [4, 4096, 14336], P('dp', 'row', 'col')
- q_factor: float32 [14336, 128], P('col')
The draws below stay inside these ranges and needn't reach their ends.
All inputs are finite; a program needn't handle non-finite values.
Results may differ from the reference program's by a relative error of at most 0.001.
Values sent between devices are 32-bit elements; how exact they have to be, the bound alone decides.
A program may use at most 128 MiB of HBM per device.

```python
import jax
import jax.numpy as jnp
from jax import lax

ROWS = 4096
COLS = 14336
RANK = 128
ITERS = 2
N_DP = 4


def block_scale(key, shape, cuts, smallest, largest):
    gain = 1.0
    for position, shards_of in cuts:
        heights = jax.random.uniform(jax.random.fold_in(jax.random.fold_in(key, 6), position), (shards_of,), jnp.float32, smallest / len(cuts), largest / len(cuts))
        gain = gain * jnp.repeat(jnp.exp(heights), shape[position] // shards_of).reshape((-1,) + (1,) * (len(shape) - 1 - position))
    return gain


def gaussian(key, dims, width, bound, shards=(), kind=jnp.bfloat16):
    level = block_scale(key, dims, shards, -0.22, 0.18) if shards else 1.0
    array = jax.random.normal(key, dims, jnp.float32) * width * level
    return jnp.minimum(jnp.maximum(array, -bound), bound).astype(kind)


def setup_inputs(seed: int = 0) -> dict:
    keys = jax.random.split(jax.random.key(seed), 4)
    grad = gaussian(keys[0], (N_DP, ROWS, COLS), 1.0, 6.0, ((0, 4), (1, 2), (2, 4)))
    error = gaussian(keys[1], (N_DP, ROWS, COLS), 0.5, 6.0, ((0, 4), (1, 2), (2, 4)))
    q_init = gaussian(keys[2], (COLS, RANK), 1.0, 6.0, ((0, 4),), jnp.float32)
    return dict(grad=grad, error=error, q_init=q_init)


def orthonormal(p_mat):
    gram = jnp.dot(p_mat.T.astype(jnp.float32), p_mat.astype(jnp.float32), precision=lax.Precision.HIGHEST, preferred_element_type=jnp.float32)
    lower = jnp.linalg.cholesky(gram)
    return jax.scipy.linalg.solve_triangular(lower, p_mat.T, lower=True).T

def reference(grad, error, q_init):
    workers = grad.shape[0]
    q_mat = q_init
    p_hat = None
    for step in range(ITERS):
        p_mat = jnp.zeros((grad.shape[1], q_mat.shape[1]), jnp.float32)
        for worker in range(workers):
            comp = grad[worker].astype(jnp.float32) + error[worker].astype(jnp.float32)
            p_mat = p_mat + jnp.dot(comp.astype(jnp.float32), q_mat.astype(jnp.float32), precision=lax.Precision.HIGHEST, preferred_element_type=jnp.float32)
        p_hat = orthonormal(p_mat * (1.0 / workers))
        q_next = jnp.zeros(q_mat.shape, jnp.float32)
        for worker in range(workers):
            comp = grad[worker].astype(jnp.float32) + error[worker].astype(jnp.float32)
            q_next = q_next + jnp.dot(comp.T.astype(jnp.float32), p_hat.astype(jnp.float32), precision=lax.Precision.HIGHEST, preferred_element_type=jnp.float32)
        q_mat = q_next * (1.0 / workers)
    approx = jnp.dot(p_hat.astype(jnp.float32), q_mat.T.astype(jnp.float32), precision=lax.Precision.HIGHEST, preferred_element_type=jnp.float32)
    comp_all = grad.astype(jnp.float32) + error.astype(jnp.float32)
    new_error = (comp_all - approx[None]).astype(jnp.bfloat16)
    return (new_error, q_mat)
```

```python
import functools

import jax
import jax.numpy as jnp
from jax import lax
from jax.experimental import pallas as pl
from jax.experimental.pallas import tpu as pltpu
from jax.sharding import PartitionSpec as P

ITERS = 2


def power_of_two(n):
    return n & (n - 1) == 0


def exchange(value, axis, bit):
    n = lax.axis_size(axis)
    return lax.ppermute(value, axis, [(i, i ^ bit) for i in range(n)])


def bits_of(axes):
    steps = []
    for axis in axes:
        bit = 1
        while bit < lax.axis_size(axis):
            steps.append((axis, bit))
            bit *= 2
    return steps


def upper(axis, bit):
    return lax.rem(lax.axis_index(axis) // bit, 2)


def butterfly(values_axes):
    state = [(value, bits_of(axes)) for value, axes in values_axes]
    values = [value for value, _ in state]
    depth = len(state[0][1])
    for level in range(depth):
        for k, (_, steps) in enumerate(state):
            axis, bit = steps[level]
            half = values[k].shape[0] // 2
            side = upper(axis, bit)
            keep = lax.dynamic_slice_in_dim(values[k], side * half, half, 0)
            give = lax.dynamic_slice_in_dim(values[k], (1 - side) * half, half, 0)
            values[k] = keep + exchange(give, axis, bit)
    for level in reversed(range(depth)):
        for k, (_, steps) in enumerate(state):
            axis, bit = steps[level]
            first = upper(axis, bit) == 0
            mine = values[k]
            other = exchange(mine, axis, bit)
            values[k] = jnp.concatenate(
                [jnp.where(first, mine, other), jnp.where(first, other, mine)], axis=0
            )
    return values


def reduce_over(value, axis_a, axis_b):
    sizes = lax.axis_size(axis_a), lax.axis_size(axis_b)
    rows = value.shape[0]
    if not all(map(power_of_two, sizes)) or rows % (2 * sizes[0] * sizes[1]):
        return lax.psum(value, (axis_a, axis_b))
    half = rows // 2
    parts = butterfly(
        [(value[:half], (axis_a, axis_b)), (value[half:], (axis_b, axis_a))]
    )
    return jnp.concatenate(parts, axis=0)


def reduce_small(value, axis):
    if not power_of_two(lax.axis_size(axis)):
        return lax.psum(value, axis)
    for name, bit in bits_of((axis,)):
        value = value + exchange(value, name, bit)
    return value


def split(value):
    high = lax.reduce_precision(value, exponent_bits=8, mantissa_bits=7)
    return high.astype(jnp.bfloat16), (value - high).astype(jnp.bfloat16)


def product(high, low, factor, side):
    rank = factor.shape[1]
    both = jnp.concatenate(split(factor), axis=1)
    dims = (((side,), (0,)), ((), ()))
    total = lax.dot_general(high, both, dims, preferred_element_type=jnp.float32)
    total = total + lax.dot_general(low, both, dims, preferred_element_type=jnp.float32)
    return total[:, :rank] + total[:, rank:]


def exact_dot(a, b, dims):
    return lax.dot_general(
        a, b, (dims, ((), ())), precision=lax.Precision.HIGHEST,
        preferred_element_type=jnp.float32,
    )


def shards(grad, error, q_init):
    comp = grad[0].astype(jnp.float32) + error[0].astype(jnp.float32)
    high, low = lax.optimization_barrier(split(comp))
    scale = 1.0 / lax.axis_size("dp")
    q_mat = q_init
    p_hat = None
    eye = jnp.eye(q_init.shape[1], dtype=jnp.float32)
    for step in range(ITERS):
        p_mat = reduce_over(product(high, low, q_mat, 1), "col", "dp") * scale
        gram = reduce_small(exact_dot(p_mat, p_mat, ((0,), (0,))), "row")
        term = reduce_over(product(high, low, p_mat, 0), "row", "dp") * scale
        lower = jnp.linalg.cholesky(gram)
        inverse = jax.scipy.linalg.solve_triangular(lower, eye, lower=True)
        q_mat = exact_dot(term, inverse, ((1,), (1,)))
        p_hat = exact_dot(p_mat, inverse, ((1,), (1,)))
    p_high, p_low = split(p_hat)
    q_high, q_low = split(q_mat)
    left = jnp.concatenate([p_high, p_high, p_low], axis=1)
    right = jnp.concatenate([q_high, q_low, q_high], axis=1)
    approx = lax.dot_general(
        left, right, (((1,), (1,)), ((), ())), preferred_element_type=jnp.float32
    )
    comp = grad[0].astype(jnp.float32) + error[0].astype(jnp.float32)
    new_error = (comp - approx).astype(jnp.bfloat16)[None]
    return (new_error, q_mat)


MESH = pl.DeviceIdType.MESH
CHUNK_ROWS = 256
CHUNK_COLS = 256
LAG_P = 2
LAG_Q = 2


def split_bf16(value):
    high = value.astype(jnp.bfloat16)
    low = (value - high.astype(jnp.float32)).astype(jnp.bfloat16)
    return high, low


def dot(a, b, side_a, side_b):
    return lax.dot_general(
        a, b, (((side_a,), (side_b,)), ((), ())), preferred_element_type=jnp.float32
    )


class Plan:
    def __init__(self, mesh, rows, cols, rank):
        self.rows, self.cols, self.rank = rows, cols, rank
        self.n_dp, self.n_row = mesh["dp"], mesh["row"]
        self.n_pair = 2
        self.n_far = mesh["col"] // 2
        self.p_rows, self.q_cols = CHUNK_ROWS, CHUNK_COLS
        self.p_chunks, self.q_chunks = rows // self.p_rows, cols // self.q_cols
        self.p_pair = self.p_rows // self.n_pair
        self.p_far = self.p_pair // max(self.n_far, 1)
        self.p_dp = self.p_far // self.n_dp
        self.q_row = rank // self.n_row
        self.q_dp = self.q_row // self.n_dp

    def fits(self, mesh):
        return (
            mesh["col"] % 2 == 0
            and min(self.n_dp, self.n_row, self.n_far) > 1
            and self.rank == 128
            and self.rows % self.p_rows == 0
            and self.cols % self.q_cols == 0
            and self.p_dp % 8 == 0
            and self.q_dp % 8 == 0
            and self.p_far * self.n_far * self.n_pair == self.p_rows
            and self.p_dp * self.n_dp == self.p_far
            and self.q_dp * self.n_dp * self.n_row == self.rank
            and self.rows * self.cols * 4 <= 30 << 20
        )


def iterate_kernel(
    plan, g_hbm, e_hbm, q_in,
    left_out, q_out, factor,
    g, e, p_t, p_sum, p_all, q_sum, q_all,
    pair_in, far_in, p_dp_in, row_in, q_dp_in,
    gram, gram_in, work, inverse,
    load_sem, gram_sem, pair_sem, far_sem, pdp_sem, pdp2_sem, far2_sem, pair2_sem,
    row_sem, qdp_sem, qdp2_sem, row2_sem,
):
    rank = plan.rank
    z, x, col = lax.axis_index("dp"), lax.axis_index("row"), lax.axis_index("col")
    core, y = lax.rem(col, 2), col // 2
    peers = {
        "pair": [(col, {"col": y * 2 + 1 - core}, 1 - core)],
        "far": [], "dp": [], "row": [],
    }
    for d in range(1, plan.n_far):
        t = lax.rem(y + d, plan.n_far)
        peers["far"].append((d, {"col": t * 2 + core}, t))
    for d in range(1, plan.n_dp):
        t = lax.rem(z + d, plan.n_dp)
        peers["dp"].append((d, {"dp": t}, t))
    for d in range(1, plan.n_row):
        t = lax.rem(x + d, plan.n_row)
        peers["row"].append((d, {"row": t}, t))
    everyone = [p for name in ("pair", "far", "dp", "row") for p in peers[name]]

    def load(c):
        rows = pl.ds(pl.multiple_of(c * plan.p_rows, plan.p_rows), plan.p_rows)
        return (
            pltpu.make_async_copy(g_hbm.at[0, rows], g.at[rows], load_sem.at[0, c]),
            pltpu.make_async_copy(e_hbm.at[0, rows], e.at[rows], load_sem.at[1, c]),
        )

    @pl.loop(0, plan.p_chunks)
    def _(c):
        for copy in load(c):
            copy.start()

    barrier = pltpu.get_barrier_semaphore()
    for _, device, _ in everyone:
        pl.semaphore_signal(barrier, inc=1, device_id=device, device_id_type=MESH)
    pl.semaphore_wait(barrier, len(everyone))

    @pl.loop(0, plan.q_chunks)
    def _(c):
        rows = pl.ds(pl.multiple_of(c * plan.q_cols, plan.q_cols), plan.q_cols)
        high, low = split_bf16(q_in[rows, :])
        factor[rows, :rank] = high
        factor[rows, rank:] = low

    def remote(src, dst, sems, index, device):
        return pltpu.make_async_remote_copy(
            src_ref=src, dst_ref=dst,
            send_sem=sems.at[(0,) + index], recv_sem=sems.at[(1,) + index],
            device_id=device, device_id_type=MESH,
        )

    def p_slice(c, *parts):
        start, size = c * plan.p_rows, plan.p_rows
        for part, width in zip(parts, (plan.p_pair, plan.p_far, plan.p_dp)):
            start, size = start + part * width, width
        return pl.ds(pl.multiple_of(start, 8), size)

    def small(c, size):
        return pl.ds(pl.multiple_of(c * size, 8), size)

    def pair_rs(c):
        return [
            remote(p_sum.at[p_slice(c, t)], pair_in.at[small(c, plan.p_pair)], pair_sem, (c,), dev)
            for _, dev, t in peers["pair"]
        ]

    def far_rs(c):
        return [
            remote(p_sum.at[p_slice(c, core, t)], far_in.at[d - 1, small(c, plan.p_far)], far_sem, (c, d - 1), dev)
            for d, dev, t in peers["far"]
        ]

    def pdp_rs(c):
        return [
            remote(p_sum.at[p_slice(c, core, y, t)], p_dp_in.at[d - 1, small(c, plan.p_dp)], pdp_sem, (c, d - 1), dev)
            for d, dev, t in peers["dp"]
        ]

    def pdp_ag(c):
        mine = p_slice(c, core, y, z)
        return [remote(p_all.at[mine], p_all.at[mine], pdp2_sem, (c, d - 1), dev) for d, dev, _ in peers["dp"]]

    def far_ag(c):
        mine = p_slice(c, core, y)
        return [remote(p_all.at[mine], p_all.at[mine], far2_sem, (c, d - 1), dev) for d, dev, _ in peers["far"]]

    def pair_ag(c):
        mine = p_slice(c, core)
        return [remote(p_all.at[mine], p_all.at[mine], pair2_sem, (c,), dev) for _, dev, _ in peers["pair"]]

    def q_slice(part, dp_part=None):
        if dp_part is None:
            return pl.ds(pl.multiple_of(part * plan.q_row, 8), plan.q_row)
        return pl.ds(pl.multiple_of(part * plan.q_row + dp_part * plan.q_dp, 8), plan.q_dp)

    def row_rs(c):
        return [
            remote(q_sum.at[c, q_slice(t)], row_in.at[d - 1, c], row_sem, (c, d - 1), dev)
            for d, dev, t in peers["row"]
        ]

    def qdp_rs(c):
        return [
            remote(q_sum.at[c, q_slice(x, t)], q_dp_in.at[d - 1, c], qdp_sem, (c, d - 1), dev)
            for d, dev, t in peers["dp"]
        ]

    def qdp_ag(c):
        mine = q_slice(x, z)
        return [remote(q_all.at[c, mine], q_all.at[c, mine], qdp2_sem, (c, d - 1), dev) for d, dev, _ in peers["dp"]]

    def row_ag(c):
        mine = q_slice(x)
        return [remote(q_all.at[c, mine], q_all.at[c, mine], row2_sem, (c, d - 1), dev) for d, dev, _ in peers["row"]]

    def start(copies):
        for copy in copies:
            copy.start()

    def wait(copies):
        for copy in copies:
            copy.wait()

    scale = 1.0 / plan.n_dp

    def stage(t, lag, index, chunks, body):
        c = t - lag * index
        @pl.when((c >= 0) & (c < chunks))
        def _():
            body(c)

    def gram_copies():
        return [
            remote(gram, gram_in.at[d - 1], gram_sem, (d - 1,), dev) for d, dev, _ in peers["row"]
        ]

    lanes = lax.broadcasted_iota(jnp.int32, (rank, rank), 1)
    sublanes = lax.broadcasted_iota(jnp.int32, (rank, rank), 0)
    per_step = -(-rank // (4 * LAG_Q - 2))

    def eliminate(j):
        row = work[pl.ds(j, 1), :]
        unit = inverse[pl.ds(j, 1), :]
        square = work[...]
        column = jnp.sum(jnp.where(lanes == j, square, 0.0), axis=1, keepdims=True)
        pivot = jnp.sum(jnp.where(lanes[:1] == j, row, 0.0), axis=1, keepdims=True)
        ratio = jnp.where(sublanes[:, :1] > j, column * (1.0 / pivot), 0.0)
        work[...] = square - ratio * row
        inverse[...] = inverse[...] - ratio * unit

    @pl.loop(0, ITERS)
    def _(step):
        def p_make(c):
            @pl.when(step == 0)
            def _():
                wait(load(c))
            rows = p_slice(c)
            both = dot(g[rows, :], factor[...], 1, 0) + dot(e[rows, :], factor[...], 1, 0)
            p_sum[rows, :] = both[:, :rank] + both[:, rank:]
            start(pair_rs(c))

        def p_pair(c):
            wait(pair_rs(c))
            rows = p_slice(c, core)
            p_sum[rows, :] = p_sum[rows, :] + pair_in[small(c, plan.p_pair), :]
            start(far_rs(c))

        def p_far(c):
            wait(far_rs(c))
            rows = p_slice(c, core, y)
            total = p_sum[rows, :]
            for d, _, _ in peers["far"]:
                total = total + far_in[d - 1, small(c, plan.p_far), :]
            p_sum[rows, :] = total
            start(pdp_rs(c))

        def p_dp(c):
            wait(pdp_rs(c))
            rows = p_slice(c, core, y, z)
            total = p_sum[rows, :]
            for d, _, _ in peers["dp"]:
                total = total + p_dp_in[d - 1, small(c, plan.p_dp), :]
            p_all[rows, :] = total * scale
            start(pdp_ag(c))

        def p_far2(c):
            wait(pdp_ag(c))
            start(far_ag(c))

        def p_pair2(c):
            wait(far_ag(c))
            start(pair_ag(c))

        def p_use(c):
            wait(pair_ag(c))
            for part in range(plan.p_rows // 128):
                rows = pl.ds(pl.multiple_of(c * plan.p_rows + part * 128, 128), 128)
                high, low = split_bf16(jnp.transpose(p_all[rows, :]))
                p_t[:rank, rows] = high
                p_t[rank:, rows] = low

        @pl.loop(0, plan.p_chunks + 6 * LAG_P)
        def _(t):
            for index, body in enumerate((p_make, p_pair, p_far, p_dp, p_far2, p_pair2, p_use)):
                stage(t, LAG_P, index, plan.p_chunks, body)

        square = dot(p_t[...], p_t[...], 1, 1)
        gram[...] = square[:rank, :rank] + square[:rank, rank:] + square[rank:, :rank] + square[rank:, rank:]
        start(gram_copies())

        def q_make(c):
            cols = pl.ds(pl.multiple_of(c * plan.q_cols, plan.q_cols), plan.q_cols)
            both = dot(p_t[...], g[:, cols], 1, 0) + dot(p_t[...], e[:, cols], 1, 0)
            q_sum[c] = both[:rank] + both[rank:]
            start(row_rs(c))

        def q_row(c):
            wait(row_rs(c))
            mine = q_slice(x)
            total = q_sum[c, mine, :]
            for d, _, _ in peers["row"]:
                total = total + row_in[d - 1, c]
            q_sum[c, mine, :] = total
            start(qdp_rs(c))

        def q_dp(c):
            wait(qdp_rs(c))
            mine = q_slice(x, z)
            total = q_sum[c, mine, :]
            for d, _, _ in peers["dp"]:
                total = total + q_dp_in[d - 1, c]
            q_all[c, mine, :] = total * scale
            start(qdp_ag(c))

        def q_row2(c):
            wait(qdp_ag(c))
            start(row_ag(c))

        def q_use(c):
            wait(row_ag(c))
            rows = pl.ds(pl.multiple_of(c * plan.q_cols, plan.q_cols), plan.q_cols)
            value = lax.dot_general(
                jnp.transpose(q_all[c]), inverse[...], (((1,), (1,)), ((), ())),
                precision=lax.Precision.HIGHEST, preferred_element_type=jnp.float32,
            )
            q_out[rows, :] = value
            high, low = split_bf16(value)
            factor[rows, :rank] = high
            factor[rows, rank:] = low

        def p_hat(c):
            rows = p_slice(c)
            value = lax.dot_general(
                p_all[rows, :], inverse[...], (((1,), (1,)), ((), ())),
                precision=lax.Precision.HIGHEST, preferred_element_type=jnp.float32,
            )
            high, low = split_bf16(value)
            left_out[rows, :rank] = high
            left_out[rows, rank:] = low

        @pl.loop(0, plan.q_chunks + 4 * LAG_Q)
        def _(t):
            stage(t, LAG_Q, 0, plan.q_chunks, q_make)
            stage(t, LAG_Q, 1, plan.q_chunks, q_row)
            stage(t, LAG_Q, 2, plan.q_chunks, q_dp)
            stage(t, LAG_Q, 3, plan.q_chunks, q_row2)

            @pl.when(t == 2)
            def _():
                wait(gram_copies())
                total = gram[...]
                for d, _, _ in peers["row"]:
                    total = total + gram_in[d - 1]
                work[...] = total
                inverse[...] = jnp.where(lanes == sublanes, 1.0, 0.0)

            @pl.when((t >= 2) & (t < 4 * LAG_Q))
            def _():
                first = (t - 2) * per_step

                @pl.loop(first, jnp.minimum(first + per_step, rank))
                def _(j):
                    eliminate(j)

            @pl.when(t == 4 * LAG_Q - 1)
            def _():
                diagonal = jnp.sum(jnp.where(lanes == sublanes, work[...], 0.0), axis=1, keepdims=True)
                inverse[...] = inverse[...] / jnp.sqrt(diagonal)

            stage(t, LAG_Q, 4, plan.q_chunks, q_use)

            @pl.when(step == ITERS - 1)
            def _():
                stage(t, LAG_Q, 4, plan.p_chunks, p_hat)


def output_kernel(g, e, left, factor, q_in, new_error, q_out):
    @pl.when(pl.program_id(0) == 0)
    def _():
        q_out[...] = q_in[...]

    rank = left.shape[1] // 2
    first = left[...]
    second = jnp.concatenate([first[:, rank:], first[:, :rank]], axis=1)
    cols = factor.shape[0]
    width = CHUNK_COLS * 2 if cols % (CHUNK_COLS * 2) == 0 else cols
    for start in range(0, cols, width):
        part = slice(start, start + width)
        right = factor[part, :]
        approx = dot(first, right, 1, 1) + dot(second, right, 1, 1)
        comp = g[0, :, part].astype(jnp.float32) + e[0, :, part].astype(jnp.float32)
        new_error[0, :, part] = (comp - approx).astype(jnp.bfloat16)


def fused(plan, grad, error, q_init):
    rows, cols, rank = plan.rows, plan.cols, plan.rank
    pc, qc = plan.p_chunks, plan.q_chunks
    f32, bf16 = jnp.float32, jnp.bfloat16
    dma = pltpu.SemaphoreType.DMA
    dp, row, far = plan.n_dp - 1, plan.n_row - 1, plan.n_far - 1
    whole = pl.BlockSpec(memory_space=pltpu.VMEM)
    left, q_factor, factor = pl.pallas_call(
        functools.partial(iterate_kernel, plan),
        out_shape=[
            jax.ShapeDtypeStruct((rows, 2 * rank), bf16),
            jax.ShapeDtypeStruct((cols, rank), f32),
            jax.ShapeDtypeStruct((cols, 2 * rank), bf16),
        ],
        in_specs=[pl.BlockSpec(memory_space=pl.ANY)] * 2 + [whole],
        out_specs=[whole] * 3,
        scratch_shapes=[
            pltpu.VMEM((rows, cols), bf16), pltpu.VMEM((rows, cols), bf16),
            pltpu.VMEM((2 * rank, rows), bf16),
            pltpu.VMEM((rows, rank), f32), pltpu.VMEM((rows, rank), f32),
            pltpu.VMEM((qc, rank, plan.q_cols), f32), pltpu.VMEM((qc, rank, plan.q_cols), f32),
            pltpu.VMEM((pc * plan.p_pair, rank), f32),
            pltpu.VMEM((far, pc * plan.p_far, rank), f32),
            pltpu.VMEM((dp, pc * plan.p_dp, rank), f32),
            pltpu.VMEM((row, qc, plan.q_row, plan.q_cols), f32),
            pltpu.VMEM((dp, qc, plan.q_dp, plan.q_cols), f32),
            pltpu.VMEM((rank, rank), f32), pltpu.VMEM((row, rank, rank), f32),
            pltpu.VMEM((rank, rank), f32), pltpu.VMEM((rank, rank), f32),
            dma((2, pc)), dma((2, row)), dma((2, pc)), dma((2, pc, far)),
            dma((2, pc, dp)), dma((2, pc, dp)), dma((2, pc, far)), dma((2, pc)),
            dma((2, qc, row)), dma((2, qc, dp)), dma((2, qc, dp)), dma((2, qc, row)),
        ],
        compiler_params=pltpu.CompilerParams(
            collective_id=0, has_side_effects=True, vmem_limit_bytes=60 << 20
        ),
        name="iterate",
    )(grad, error, q_init)
    block = pl.BlockSpec((1, plan.p_rows, cols), lambda i: (0, i, 0))
    return pl.pallas_call(
        output_kernel,
        grid=(pc,),
        out_shape=[
            jax.ShapeDtypeStruct((1, rows, cols), bf16),
            jax.ShapeDtypeStruct((cols, rank), f32),
        ],
        in_specs=[
            block, block,
            pl.BlockSpec((plan.p_rows, 2 * rank), lambda i: (i, 0)),
            pl.BlockSpec((cols, 2 * rank), lambda i: (0, 0)),
            pl.BlockSpec((cols, rank), lambda i: (0, 0)),
        ],
        out_specs=[block, pl.BlockSpec((cols, rank), lambda i: (0, 0))],
        compiler_params=pltpu.CompilerParams(vmem_limit_bytes=48 << 20),
        name="residual",
    )(grad, error, left, factor, q_factor)


def solution(mesh):
    in_specs = (P("dp", "row", "col"), P("dp", "row", "col"), P("col", None))
    out_specs = (P("dp", "row", "col"), P("col", None))
    sizes = dict(mesh.shape)

    def step(grad, error, q_init):
        plan = Plan(sizes, grad.shape[1], grad.shape[2], q_init.shape[1])
        if plan.fits(sizes):
            return tuple(fused(plan, grad, error, q_init))
        return shards(grad, error, q_init)

    return jax.shard_map(step, mesh=mesh, in_specs=in_specs, out_specs=out_specs, check_vma=False)
```

```python
import functools

import jax
import jax.numpy as jnp
from jax import lax
from jax.experimental import pallas as pl
from jax.experimental.pallas import tpu as pltpu
from jax.sharding import PartitionSpec as P

ITERS = 2


def power_of_two(n):
    return n & (n - 1) == 0


def exchange(value, axis, bit):
    n = lax.axis_size(axis)
    return lax.ppermute(value, axis, [(i, i ^ bit) for i in range(n)])


def bits_of(axes):
    steps = []
    for axis in axes:
        bit = 1
        while bit < lax.axis_size(axis):
            steps.append((axis, bit))
            bit *= 2
    return steps


def upper(axis, bit):
    return lax.rem(lax.axis_index(axis) // bit, 2)


def butterfly(values_axes):
    state = [(value, bits_of(axes)) for value, axes in values_axes]
    values = [value for value, _ in state]
    depth = len(state[0][1])
    for level in range(depth):
        for k, (_, steps) in enumerate(state):
            axis, bit = steps[level]
            half = values[k].shape[0] // 2
            side = upper(axis, bit)
            keep = lax.dynamic_slice_in_dim(values[k], side * half, half, 0)
            give = lax.dynamic_slice_in_dim(values[k], (1 - side) * half, half, 0)
            values[k] = keep + exchange(give, axis, bit)
    for level in reversed(range(depth)):
        for k, (_, steps) in enumerate(state):
            axis, bit = steps[level]
            first = upper(axis, bit) == 0
            mine = values[k]
            other = exchange(mine, axis, bit)
            values[k] = jnp.concatenate(
                [jnp.where(first, mine, other), jnp.where(first, other, mine)], axis=0
            )
    return values


def reduce_over(value, axis_a, axis_b):
    sizes = lax.axis_size(axis_a), lax.axis_size(axis_b)
    rows = value.shape[0]
    if not all(map(power_of_two, sizes)) or rows % (2 * sizes[0] * sizes[1]):
        return lax.psum(value, (axis_a, axis_b))
    half = rows // 2
    parts = butterfly(
        [(value[:half], (axis_a, axis_b)), (value[half:], (axis_b, axis_a))]
    )
    return jnp.concatenate(parts, axis=0)


def reduce_small(value, axis):
    if not power_of_two(lax.axis_size(axis)):
        return lax.psum(value, axis)
    for name, bit in bits_of((axis,)):
        value = value + exchange(value, name, bit)
    return value


def split(value):
    high = lax.reduce_precision(value, exponent_bits=8, mantissa_bits=7)
    return high.astype(jnp.bfloat16), (value - high).astype(jnp.bfloat16)


def product(high, low, factor, side):
    rank = factor.shape[1]
    both = jnp.concatenate(split(factor), axis=1)
    dims = (((side,), (0,)), ((), ()))
    total = lax.dot_general(high, both, dims, preferred_element_type=jnp.float32)
    total = total + lax.dot_general(low, both, dims, preferred_element_type=jnp.float32)
    return total[:, :rank] + total[:, rank:]


def exact_dot(a, b, dims):
    return lax.dot_general(
        a, b, (dims, ((), ())), precision=lax.Precision.HIGHEST,
        preferred_element_type=jnp.float32,
    )


def shards(grad, error, q_init):
    comp = grad[0].astype(jnp.float32) + error[0].astype(jnp.float32)
    high, low = lax.optimization_barrier(split(comp))
    scale = 1.0 / lax.axis_size("dp")
    q_mat = q_init
    p_hat = None
    eye = jnp.eye(q_init.shape[1], dtype=jnp.float32)
    for step in range(ITERS):
        p_mat = reduce_over(product(high, low, q_mat, 1), "col", "dp") * scale
        gram = reduce_small(exact_dot(p_mat, p_mat, ((0,), (0,))), "row")
        term = reduce_over(product(high, low, p_mat, 0), "row", "dp") * scale
        lower = jnp.linalg.cholesky(gram)
        inverse = jax.scipy.linalg.solve_triangular(lower, eye, lower=True)
        q_mat = exact_dot(term, inverse, ((1,), (1,)))
        p_hat = exact_dot(p_mat, inverse, ((1,), (1,)))
    p_high, p_low = split(p_hat)
    q_high, q_low = split(q_mat)
    left = jnp.concatenate([p_high, p_high, p_low], axis=1)
    right = jnp.concatenate([q_high, q_low, q_high], axis=1)
    approx = lax.dot_general(
        left, right, (((1,), (1,)), ((), ())), preferred_element_type=jnp.float32
    )
    comp = grad[0].astype(jnp.float32) + error[0].astype(jnp.float32)
    new_error = (comp - approx).astype(jnp.bfloat16)[None]
    return (new_error, q_mat)


MESH = pl.DeviceIdType.MESH
CHUNK_ROWS = 256
CHUNK_COLS = 256
LAG_P = 3
LAG_Q = 2
USE_Q = 13
STEPS_P_HAT = 2
RESIDUAL_ROWS = 512
VMEM_BYTES = 45 << 20


def split_bf16(value):
    high = value.astype(jnp.bfloat16)
    low = (value - high.astype(jnp.float32)).astype(jnp.bfloat16)
    return high, low


def dot(a, b, side_a, side_b):
    return lax.dot_general(
        a, b, (((side_a,), (side_b,)), ((), ())), preferred_element_type=jnp.float32
    )


class Plan:
    def __init__(self, mesh, rows, cols, rank):
        self.rows, self.cols, self.rank = rows, cols, rank
        self.n_dp, self.n_row = mesh["dp"], mesh["row"]
        self.n_pair = 2
        self.n_far = mesh["col"] // 2
        self.p_rows, self.q_cols = CHUNK_ROWS, CHUNK_COLS
        self.p_chunks, self.q_chunks = rows // self.p_rows, cols // self.q_cols
        self.p_pair = self.p_rows // self.n_pair
        self.p_far = self.p_pair // max(self.n_far, 1)
        self.p_dp = self.p_far // self.n_dp
        self.q_row = rank // self.n_row
        self.q_half = rank // 2

    def fits(self, mesh):
        return (
            mesh["col"] % 2 == 0
            and self.n_dp == 4
            and self.n_far > 1
            and self.rank == 128
            and self.rows % self.p_rows == 0
            and self.cols % self.q_cols == 0
            and self.p_dp % 8 == 0
            and self.q_row % 8 == 0
            and self.n_row == 2
            and self.rows % RESIDUAL_ROWS == 0
            and self.p_far * self.n_far * self.n_pair == self.p_rows
            and self.p_dp * self.n_dp == self.p_far
            and self.q_row * self.n_row == self.rank
            and self.rows * self.cols * 4 <= 30 << 20
        )


def iterate_kernel(
    plan, g_hbm, e_hbm, q_in,
    g, q_out,
    e, factor, left, p_t, p_sum, p_all, q_sum, q_all,
    pair_in, far_in, p_dp_in, row_in, up_in, up_out, down_in, down_out, end_in, mid_in,
    gram, gram_in, work, inverse,
    load_sem, gram_sem, pair_sem, far_sem, pdp_sem, pdp2_sem, far2_sem, pair2_sem,
    row_sem, row2_sem, up_sem, down_sem, end_sem, mid_sem, cross_sem, near_sem, far_out_sem,
):
    rank = plan.rank
    z, x, col = lax.axis_index("dp"), lax.axis_index("row"), lax.axis_index("col")
    core, y = lax.rem(col, 2), col // 2
    peers = {
        "pair": [(col, {"col": y * 2 + 1 - core}, 1 - core)],
        "far": [], "dp": [], "row": [],
    }
    for d in range(1, plan.n_far):
        t = lax.rem(y + d, plan.n_far)
        peers["far"].append((d, {"col": t * 2 + core}, t))
    for d in range(1, plan.n_dp):
        t = lax.rem(z + d, plan.n_dp)
        peers["dp"].append((d, {"dp": t}, t))
    for d in range(1, plan.n_row):
        t = lax.rem(x + d, plan.n_row)
        peers["row"].append((d, {"row": t}, t))
    everyone = [p for name in ("pair", "far", "dp", "row") for p in peers[name]]

    def load(c):
        rows = pl.ds(pl.multiple_of(c * plan.p_rows, plan.p_rows), plan.p_rows)
        return (
            pltpu.make_async_copy(g_hbm.at[0, rows], g.at[0, rows], load_sem.at[0, c]),
            pltpu.make_async_copy(e_hbm.at[0, rows], e.at[rows], load_sem.at[1, c]),
        )

    @pl.loop(0, plan.p_chunks)
    def _(c):
        for copy in load(c):
            copy.start()

    barrier = pltpu.get_barrier_semaphore()
    for _, device, _ in everyone:
        pl.semaphore_signal(barrier, inc=1, device_id=device, device_id_type=MESH)
    pl.semaphore_wait(barrier, len(everyone))

    @pl.loop(0, plan.q_chunks)
    def _(c):
        rows = pl.ds(pl.multiple_of(c * plan.q_cols, plan.q_cols), plan.q_cols)
        high, low = split_bf16(q_in[rows, :])
        factor[rows, :rank] = high
        factor[rows, rank:] = low

    def remote(src, dst, sems, index, device):
        return pltpu.make_async_remote_copy(
            src_ref=src, dst_ref=dst,
            send_sem=sems.at[(0,) + index], recv_sem=sems.at[(1,) + index],
            device_id=device, device_id_type=MESH,
        )

    def p_slice(c, *parts):
        start, size = c * plan.p_rows, plan.p_rows
        for part, width in zip(parts, (plan.p_pair, plan.p_far, plan.p_dp)):
            start, size = start + part * width, width
        return pl.ds(pl.multiple_of(start, 8), size)

    def small(c, size):
        return pl.ds(pl.multiple_of(c * size, 8), size)

    def pair_rs(c):
        return [
            remote(p_sum.at[p_slice(c, t)], pair_in.at[small(c, plan.p_pair)], pair_sem, (c,), dev)
            for _, dev, t in peers["pair"]
        ]

    def far_rs(c):
        return [
            remote(p_sum.at[p_slice(c, core, t)], far_in.at[d - 1, small(c, plan.p_far)], far_sem, (c, d - 1), dev)
            for d, dev, t in peers["far"]
        ]

    def pdp_rs(c):
        return [
            remote(p_sum.at[p_slice(c, core, y, t)], p_dp_in.at[d - 1, small(c, plan.p_dp)], pdp_sem, (c, d - 1), dev)
            for d, dev, t in peers["dp"]
        ]

    def pdp_ag(c):
        mine = p_slice(c, core, y, z)
        return [remote(p_all.at[mine], p_all.at[mine], pdp2_sem, (c, d - 1), dev) for d, dev, _ in peers["dp"]]

    def far_ag(c):
        mine = p_slice(c, core, y)
        return [remote(p_all.at[mine], p_all.at[mine], far2_sem, (c, d - 1), dev) for d, dev, _ in peers["far"]]

    def pair_ag(c):
        mine = p_slice(c, core)
        return [remote(p_all.at[mine], p_all.at[mine], pair2_sem, (c,), dev) for _, dev, _ in peers["pair"]]

    def q_slice(part):
        return pl.ds(pl.multiple_of(part * plan.q_row, 8), plan.q_row)

    side = z // 2
    inner = (z == 1) | (z == 2)
    near, far_half = pl.ds(pl.multiple_of(side * plan.q_half, 8), plan.q_half), pl.ds(
        pl.multiple_of((1 - side) * plan.q_half, 8), plan.q_half
    )
    opposite = {"dp": 3 - z}
    towards = {"dp": jnp.where(side == 0, 1, 2)}
    outwards = {"dp": jnp.where(side == 0, 0, 3)}
    above, below = {"dp": jnp.minimum(z + 1, 3)}, {"dp": jnp.maximum(z - 1, 0)}

    def row_rs(c):
        return [
            remote(q_sum.at[c, q_slice(t)], row_in.at[d - 1, c], row_sem, (c, d - 1), dev)
            for d, dev, t in peers["row"]
        ]

    def row_ag(c):
        mine = q_slice(x)
        return [remote(q_all.at[c, mine], q_all.at[c, mine], row2_sem, (c, d - 1), dev) for d, dev, _ in peers["row"]]

    def up(c):
        return remote(up_out.at[c], up_in.at[c], up_sem, (c,), above)

    def down(c):
        return remote(down_out.at[c], down_in.at[c], down_sem, (c,), below)

    def end(c):
        return remote(q_sum.at[c], end_in.at[c], end_sem, (c,), towards)

    def middle(c):
        return remote(q_sum.at[c, far_half], mid_in.at[c], mid_sem, (c,), opposite)

    def row_swap(c):
        return [
            remote(q_sum.at[c, near], row_in.at[d - 1, c], row_sem, (c, d - 1), dev)
            for d, dev, _ in peers["row"]
        ]

    def cross(c):
        return remote(q_all.at[c, near], q_all.at[c, near], cross_sem, (c,), opposite)

    def near_out(c):
        return remote(q_all.at[c, near], q_all.at[c, near], near_sem, (c,), outwards)

    def far_out(c):
        return remote(q_all.at[c, far_half], q_all.at[c, far_half], far_out_sem, (c,), outwards)

    def cross_in(c):
        return remote(q_all.at[c, far_half], q_all.at[c, far_half], cross_sem, (c,), opposite)

    def start(copies):
        for copy in copies:
            copy.start()

    def wait(copies):
        for copy in copies:
            copy.wait()

    scale = 1.0 / plan.n_dp

    def stage(t, lag, index, chunks, body):
        c = t - lag * index
        @pl.when((c >= 0) & (c < chunks))
        def _():
            body(c)

    def gram_copies():
        return [
            remote(gram, gram_in.at[d - 1], gram_sem, (d - 1,), dev) for d, dev, _ in peers["row"]
        ]

    lanes = lax.broadcasted_iota(jnp.int32, (rank, rank), 1)
    sublanes = lax.broadcasted_iota(jnp.int32, (rank, rank), 0)
    last_pivot = USE_Q - STEPS_P_HAT
    per_step = -(-rank // (last_pivot - 2))
    hat_chunks = -(-plan.p_chunks // STEPS_P_HAT)

    def eliminate(j):
        row = work[pl.ds(j, 1), :]
        unit = inverse[pl.ds(j, 1), :]
        square = work[...]
        column = jnp.sum(jnp.where(lanes == j, square, 0.0), axis=1, keepdims=True)
        pivot = jnp.sum(jnp.where(lanes[:1] == j, row, 0.0), axis=1, keepdims=True)
        ratio = jnp.where(sublanes[:, :1] > j, column * (1.0 / pivot), 0.0)
        work[...] = square - ratio * row
        inverse[...] = inverse[...] - ratio * unit

    @pl.loop(0, ITERS)
    def _(step):
        def p_make(c):
            @pl.when(step == 0)
            def _():
                wait(load(c))
            rows = p_slice(c)
            both = dot(g[0, rows, :], factor[...], 1, 0) + dot(e[rows, :], factor[...], 1, 0)
            p_sum[rows, :] = both[:, :rank] + both[:, rank:]
            start(pair_rs(c))

        def p_pair(c):
            wait(pair_rs(c))
            rows = p_slice(c, core)
            p_sum[rows, :] = p_sum[rows, :] + pair_in[small(c, plan.p_pair), :]
            start(far_rs(c))

        def p_far(c):
            wait(far_rs(c))
            rows = p_slice(c, core, y)
            total = p_sum[rows, :]
            for d, _, _ in peers["far"]:
                total = total + far_in[d - 1, small(c, plan.p_far), :]
            p_sum[rows, :] = total
            start(pdp_rs(c))

        def p_dp(c):
            wait(pdp_rs(c))
            rows = p_slice(c, core, y, z)
            total = p_sum[rows, :]
            for d, _, _ in peers["dp"]:
                total = total + p_dp_in[d - 1, small(c, plan.p_dp), :]
            p_all[rows, :] = total * scale
            start(pdp_ag(c))

        def p_far2(c):
            wait(pdp_ag(c))
            start(far_ag(c))

        def p_pair2(c):
            wait(far_ag(c))
            start(pair_ag(c))

        def p_use(c):
            wait(pair_ag(c))
            for part in range(plan.p_rows // 128):
                rows = pl.ds(pl.multiple_of(c * plan.p_rows + part * 128, 128), 128)
                high, low = split_bf16(jnp.transpose(p_all[rows, :]))
                p_t[:rank, rows] = high
                p_t[rank:, rows] = low

        @pl.loop(0, plan.p_chunks + 6 * LAG_P)
        def _(t):
            for index, body in enumerate((p_make, p_pair, p_far, p_dp, p_far2, p_pair2, p_use)):
                stage(t, LAG_P, index, plan.p_chunks, body)

        square = dot(p_t[...], p_t[...], 1, 1)
        gram[...] = square[:rank, :rank] + square[:rank, rank:] + square[rank:, :rank] + square[rank:, rank:]
        start(gram_copies())

        def even(c, condition=True):
            return (lax.rem(c, 3) != 1) & condition

        def odd(c, condition=True):
            return (lax.rem(c, 3) == 1) & condition

        def q_make(c):
            cols = pl.ds(pl.multiple_of(c * plan.q_cols, plan.q_cols), plan.q_cols)
            both = dot(p_t[...], g[0, :, cols], 1, 0) + dot(p_t[...], e[:, cols], 1, 0)
            q_sum[c] = both[:rank] + both[rank:]

            @pl.when(even(c))
            def _():
                start(row_rs(c))

            @pl.when(odd(c, jnp.logical_not(inner)))
            def _():
                end(c).start()

        def q_first(c):
            @pl.when(even(c))
            def _():
                wait(row_rs(c))
                mine = q_slice(x)
                total = q_sum[c, mine, :]
                for d, _, _ in peers["row"]:
                    total = total + row_in[d - 1, c]
                q_sum[c, mine, :] = total

                @pl.when(z == 0)
                def _():
                    up_out[c] = total
                    up(c).start()

                @pl.when(z == 3)
                def _():
                    down_out[c] = total
                    down(c).start()

            @pl.when(odd(c, inner))
            def _():
                end(c).wait_recv()
                q_sum[c] = q_sum[c] + end_in[c]
                middle(c).start()

        def q_up(c):
            @pl.when(even(c, z > 0))
            def _():
                up(c).wait_recv()
                up_out[c] = up_in[c] + q_sum[c, q_slice(x), :]

                @pl.when(z < 3)
                def _():
                    up(c).start()

        def q_down(c):
            @pl.when(even(c, z < 3))
            def _():
                down(c).wait_recv()

                @pl.when(z > 0)
                def _():
                    down_out[c] = down_in[c] + q_sum[c, q_slice(x), :]
                    down(c).start()

        def q_second(c):
            @pl.when(odd(c, inner))
            def _():
                middle(c).wait_recv()
                q_sum[c, near, :] = q_sum[c, near, :] + mid_in[c]
                start(row_swap(c))

        def q_third(c):
            @pl.when(odd(c, inner))
            def _():
                wait(row_swap(c))
                total = q_sum[c, near, :]
                for d, _, _ in peers["row"]:
                    total = total + row_in[d - 1, c]
                q_all[c, near, :] = total * scale
                near_out(c).start()
                cross(c).start()

        def q_fourth(c):
            @pl.when(even(c))
            def _():
                mine = q_slice(x)

                @pl.when(z == 0)
                def _():
                    q_all[c, mine, :] = (q_sum[c, mine, :] + down_in[c]) * scale

                @pl.when(inner)
                def _():
                    q_all[c, mine, :] = (up_out[c] + down_in[c]) * scale

                @pl.when(z == 3)
                def _():
                    q_all[c, mine, :] = up_out[c] * scale

                start(row_ag(c))

            @pl.when(odd(c, inner))
            def _():
                cross_in(c).wait_recv()
                far_out(c).start()

            @pl.when(odd(c, jnp.logical_not(inner)))
            def _():
                near_out(c).wait_recv()

        def q_fifth(c):
            @pl.when(even(c))
            def _():
                wait(row_ag(c))

                @pl.when(z < 3)
                def _():
                    up(c).wait_send()

                @pl.when(z > 0)
                def _():
                    down(c).wait_send()

            @pl.when(odd(c, inner))
            def _():
                middle(c).wait_send()
                near_out(c).wait_send()
                cross(c).wait_send()
                far_out(c).wait_send()

            @pl.when(odd(c, jnp.logical_not(inner)))
            def _():
                end(c).wait_send()
                far_out(c).wait_recv()

        def q_use(c):
            rows = pl.ds(pl.multiple_of(c * plan.q_cols, plan.q_cols), plan.q_cols)
            value = lax.dot_general(
                jnp.transpose(q_all[c]), inverse[...], (((1,), (1,)), ((), ())),
                precision=lax.Precision.HIGHEST, preferred_element_type=jnp.float32,
            )
            q_out[rows, :] = value
            high, low = split_bf16(value)
            factor[rows, :rank] = high
            factor[rows, rank:] = low

            @pl.when(step == ITERS - 1)
            def _():
                right = factor[rows, :]

                @pl.loop(0, plan.rows // RESIDUAL_ROWS)
                def _(block):
                    part = pl.ds(pl.multiple_of(block * RESIDUAL_ROWS, RESIDUAL_ROWS), RESIDUAL_ROWS)
                    approx = dot(left[0, part, :], right, 1, 1) + dot(left[1, part, :], right, 1, 1)
                    comp = g[0, part, rows].astype(jnp.float32) + e[part, rows].astype(jnp.float32)
                    g[0, part, rows] = (comp - approx).astype(jnp.bfloat16)

        def p_hat(c):
            rows = p_slice(c)
            value = lax.dot_general(
                p_all[rows, :], inverse[...], (((1,), (1,)), ((), ())),
                precision=lax.Precision.HIGHEST, preferred_element_type=jnp.float32,
            )
            high, low = split_bf16(value)
            left[0, rows, :rank] = high
            left[0, rows, rank:] = low
            left[1, rows, :rank] = low
            left[1, rows, rank:] = high

        @pl.loop(0, plan.q_chunks + max(USE_Q, 5 * LAG_Q))
        def _(t):
            stage(t, LAG_Q, 0, plan.q_chunks, q_make)
            stage(t, LAG_Q, 1, plan.q_chunks, q_first)
            stage(t, LAG_Q, 1 + z, plan.q_chunks, q_up)
            stage(t, LAG_Q, 4 - z, plan.q_chunks, q_down)
            stage(t, LAG_Q, 2, plan.q_chunks, q_second)
            stage(t, LAG_Q, 3, plan.q_chunks, q_third)
            stage(t, LAG_Q, 4, plan.q_chunks, q_fourth)
            stage(t, LAG_Q, 5, plan.q_chunks, q_fifth)

            @pl.when(t == 2)
            def _():
                wait(gram_copies())
                total = gram[...]
                for d, _, _ in peers["row"]:
                    total = total + gram_in[d - 1]
                work[...] = total
                inverse[...] = jnp.where(lanes == sublanes, 1.0, 0.0)

            @pl.when((t >= 2) & (t < last_pivot))
            def _():
                first = (t - 2) * per_step

                @pl.loop(first, jnp.minimum(first + per_step, rank))
                def _(j):
                    eliminate(j)

            @pl.when(t == last_pivot)
            def _():
                diagonal = jnp.sum(jnp.where(lanes == sublanes, work[...], 0.0), axis=1, keepdims=True)
                inverse[...] = inverse[...] / jnp.sqrt(diagonal)

            @pl.when((step == ITERS - 1) & (t >= last_pivot) & (t < USE_Q))
            def _():
                first = (t - last_pivot) * hat_chunks

                @pl.loop(first, jnp.minimum(first + hat_chunks, plan.p_chunks))
                def _(c):
                    p_hat(c)

            stage(t, USE_Q, 1, plan.q_chunks, q_use)


def store_kernel(plan, residual, q_mat, new_error, q_factor, sem, q_sem):
    def blocks(c):
        rows = pl.ds(pl.multiple_of(c * plan.p_rows, plan.p_rows), plan.p_rows)
        return pltpu.make_async_copy(residual.at[0, rows], new_error.at[0, rows], sem.at[c])

    last = pltpu.make_async_copy(q_mat, q_factor, q_sem)
    for c in range(plan.p_chunks):
        blocks(c).start()
    last.start()
    for c in range(plan.p_chunks):
        blocks(c).wait()
    last.wait()


def fused(plan, grad, error, q_init):
    rows, cols, rank = plan.rows, plan.cols, plan.rank
    pc, qc = plan.p_chunks, plan.q_chunks
    f32, bf16 = jnp.float32, jnp.bfloat16
    dma = pltpu.SemaphoreType.DMA
    dp, row, far = plan.n_dp - 1, plan.n_row - 1, plan.n_far - 1
    whole = pl.BlockSpec(memory_space=pltpu.VMEM)
    part = pltpu.VMEM((qc, plan.q_row, plan.q_cols), f32)
    residual, q_mat = pl.pallas_call(
        functools.partial(iterate_kernel, plan),
        out_shape=[pltpu.VMEM((1, rows, cols), bf16), pltpu.VMEM((cols, rank), f32)],
        in_specs=[pl.BlockSpec(memory_space=pl.ANY)] * 2 + [whole],
        out_specs=[whole] * 2,
        scratch_shapes=[
            pltpu.VMEM((rows, cols), bf16),
            pltpu.VMEM((cols, 2 * rank), bf16), pltpu.VMEM((2, rows, 2 * rank), bf16),
            pltpu.VMEM((2 * rank, rows), bf16),
            pltpu.VMEM((rows, rank), f32), pltpu.VMEM((rows, rank), f32),
            pltpu.VMEM((qc, rank, plan.q_cols), f32), pltpu.VMEM((qc, rank, plan.q_cols), f32),
            pltpu.VMEM((pc * plan.p_pair, rank), f32),
            pltpu.VMEM((far, pc * plan.p_far, rank), f32),
            pltpu.VMEM((dp, pc * plan.p_dp, rank), f32),
            pltpu.VMEM((row, qc, max(plan.q_row, plan.q_half), plan.q_cols), f32),
            part, part, part, part,
            pltpu.VMEM((qc, rank, plan.q_cols), f32),
            pltpu.VMEM((qc, plan.q_half, plan.q_cols), f32),
            pltpu.VMEM((rank, rank), f32), pltpu.VMEM((row, rank, rank), f32),
            pltpu.VMEM((rank, rank), f32), pltpu.VMEM((rank, rank), f32),
            dma((2, pc)), dma((2, row)), dma((2, pc)), dma((2, pc, far)),
            dma((2, pc, dp)), dma((2, pc, dp)), dma((2, pc, far)), dma((2, pc)),
            dma((2, qc, row)), dma((2, qc, row)), dma((2, qc)), dma((2, qc)),
            dma((2, qc)), dma((2, qc)), dma((2, qc)), dma((2, qc)), dma((2, qc)),
        ],
        compiler_params=pltpu.CompilerParams(
            collective_id=0, has_side_effects=True, vmem_limit_bytes=VMEM_BYTES
        ),
        name="iterate",
    )(grad, error, q_init)
    return pl.pallas_call(
        functools.partial(store_kernel, plan),
        out_shape=[
            jax.ShapeDtypeStruct((1, rows, cols), bf16), jax.ShapeDtypeStruct((cols, rank), f32)
        ],
        in_specs=[whole] * 2,
        out_specs=[pl.BlockSpec(memory_space=pl.ANY)] * 2,
        scratch_shapes=[dma((pc,)), dma(())],
        compiler_params=pltpu.CompilerParams(vmem_limit_bytes=4 << 20),
        name="store",
    )(residual, q_mat)


def solution(mesh):
    in_specs = (P("dp", "row", "col"), P("dp", "row", "col"), P("col", None))
    out_specs = (P("dp", "row", "col"), P("col", None))
    sizes = dict(mesh.shape)

    def step(grad, error, q_init):
        plan = Plan(sizes, grad.shape[1], grad.shape[2], q_init.shape[1])
        if plan.fits(sizes):
            return tuple(fused(plan, grad, error, q_init))
        return shards(grad, error, q_init)

    return jax.shard_map(step, mesh=mesh, in_specs=in_specs, out_specs=out_specs, check_vma=False)
```

```python
import functools

import jax
import jax.numpy as jnp
from jax import lax
from jax.experimental import pallas as pl
from jax.experimental.pallas import tpu as pltpu
from jax.sharding import PartitionSpec as P

ITERS = 2


def power_of_two(n):
    return n & (n - 1) == 0


def exchange(value, axis, bit):
    n = lax.axis_size(axis)
    return lax.ppermute(value, axis, [(i, i ^ bit) for i in range(n)])


def bits_of(axes):
    steps = []
    for axis in axes:
        bit = 1
        while bit < lax.axis_size(axis):
            steps.append((axis, bit))
            bit *= 2
    return steps


def upper(axis, bit):
    return lax.rem(lax.axis_index(axis) // bit, 2)


def butterfly(values_axes):
    state = [(value, bits_of(axes)) for value, axes in values_axes]
    values = [value for value, _ in state]
    depth = len(state[0][1])
    for level in range(depth):
        for k, (_, steps) in enumerate(state):
            axis, bit = steps[level]
            half = values[k].shape[0] // 2
            side = upper(axis, bit)
            keep = lax.dynamic_slice_in_dim(values[k], side * half, half, 0)
            give = lax.dynamic_slice_in_dim(values[k], (1 - side) * half, half, 0)
            values[k] = keep + exchange(give, axis, bit)
    for level in reversed(range(depth)):
        for k, (_, steps) in enumerate(state):
            axis, bit = steps[level]
            first = upper(axis, bit) == 0
            mine = values[k]
            other = exchange(mine, axis, bit)
            values[k] = jnp.concatenate(
                [jnp.where(first, mine, other), jnp.where(first, other, mine)], axis=0
            )
    return values


def reduce_over(value, axis_a, axis_b):
    sizes = lax.axis_size(axis_a), lax.axis_size(axis_b)
    rows = value.shape[0]
    if not all(map(power_of_two, sizes)) or rows % (2 * sizes[0] * sizes[1]):
        return lax.psum(value, (axis_a, axis_b))
    half = rows // 2
    parts = butterfly(
        [(value[:half], (axis_a, axis_b)), (value[half:], (axis_b, axis_a))]
    )
    return jnp.concatenate(parts, axis=0)


def reduce_small(value, axis):
    if not power_of_two(lax.axis_size(axis)):
        return lax.psum(value, axis)
    for name, bit in bits_of((axis,)):
        value = value + exchange(value, name, bit)
    return value


def split(value):
    high = lax.reduce_precision(value, exponent_bits=8, mantissa_bits=7)
    return high.astype(jnp.bfloat16), (value - high).astype(jnp.bfloat16)


def product(high, low, factor, side):
    rank = factor.shape[1]
    both = jnp.concatenate(split(factor), axis=1)
    dims = (((side,), (0,)), ((), ()))
    total = lax.dot_general(high, both, dims, preferred_element_type=jnp.float32)
    total = total + lax.dot_general(low, both, dims, preferred_element_type=jnp.float32)
    return total[:, :rank] + total[:, rank:]


def exact_dot(a, b, dims):
    return lax.dot_general(
        a, b, (dims, ((), ())), precision=lax.Precision.HIGHEST,
        preferred_element_type=jnp.float32,
    )


def shards(grad, error, q_init):
    comp = grad[0].astype(jnp.float32) + error[0].astype(jnp.float32)
    high, low = lax.optimization_barrier(split(comp))
    scale = 1.0 / lax.axis_size("dp")
    q_mat = q_init
    p_hat = None
    eye = jnp.eye(q_init.shape[1], dtype=jnp.float32)
    for step in range(ITERS):
        p_mat = reduce_over(product(high, low, q_mat, 1), "col", "dp") * scale
        gram = reduce_small(exact_dot(p_mat, p_mat, ((0,), (0,))), "row")
        term = reduce_over(product(high, low, p_mat, 0), "row", "dp") * scale
        lower = jnp.linalg.cholesky(gram)
        inverse = jax.scipy.linalg.solve_triangular(lower, eye, lower=True)
        q_mat = exact_dot(term, inverse, ((1,), (1,)))
        p_hat = exact_dot(p_mat, inverse, ((1,), (1,)))
    p_high, p_low = split(p_hat)
    q_high, q_low = split(q_mat)
    left = jnp.concatenate([p_high, p_high, p_low], axis=1)
    right = jnp.concatenate([q_high, q_low, q_high], axis=1)
    approx = lax.dot_general(
        left, right, (((1,), (1,)), ((), ())), preferred_element_type=jnp.float32
    )
    comp = grad[0].astype(jnp.float32) + error[0].astype(jnp.float32)
    new_error = (comp - approx).astype(jnp.bfloat16)[None]
    return (new_error, q_mat)


MESH = pl.DeviceIdType.MESH
CHUNK_ROWS = 256
CHUNK_COLS = 256
LAG_P = 3
LAG_Q = 2
USE_Q = 10
STEPS_P_HAT = 2
RESIDUAL_ROWS = 1024
VMEM_BYTES = 45 << 20


def split_bf16(value):
    high = value.astype(jnp.bfloat16)
    low = (value - high.astype(jnp.float32)).astype(jnp.bfloat16)
    return high, low


def dot(a, b, side_a, side_b):
    return lax.dot_general(
        a, b, (((side_a,), (side_b,)), ((), ())), preferred_element_type=jnp.float32
    )


class Plan:
    def __init__(self, mesh, rows, cols, rank):
        self.rows, self.cols, self.rank = rows, cols, rank
        self.n_dp, self.n_row = mesh["dp"], mesh["row"]
        self.n_pair = 2
        self.n_far = mesh["col"] // 2
        self.p_rows, self.q_cols = CHUNK_ROWS, CHUNK_COLS
        self.p_chunks, self.q_chunks = rows // self.p_rows, cols // self.q_cols
        self.p_pair = self.p_rows // self.n_pair
        self.p_far = self.p_pair // max(self.n_far, 1)
        self.p_dp = self.p_far // self.n_dp
        self.q_row = rank // self.n_row
        self.q_half = rank // 2

    def fits(self, mesh):
        return (
            mesh["col"] % 2 == 0
            and self.n_dp == 4
            and self.n_far > 1
            and self.rank == 128
            and self.rows % self.p_rows == 0
            and self.cols % self.q_cols == 0
            and self.p_dp % 8 == 0
            and self.q_row % 8 == 0
            and self.n_row == 2
            and self.rows % RESIDUAL_ROWS == 0
            and self.p_far * self.n_far * self.n_pair == self.p_rows
            and self.p_dp * self.n_dp == self.p_far
            and self.q_row * self.n_row == self.rank
            and self.rows * self.cols * 4 <= 30 << 20
        )


def iterate_kernel(
    plan, g_hbm, e_hbm, q_in,
    g, q_out,
    e, factor, left, p_t, p_sum, p_all, q_sum, q_all,
    pair_in, far_in, p_dp_in, row_in, up_in, up_out, down_in, down_out, end_in, mid_in,
    gram, gram_in, work, inverse,
    load_sem, gram_sem, pair_sem, far_sem, pdp_sem, pdp2_sem, far2_sem, pair2_sem,
    row_sem, row2_sem, up_sem, down_sem, end_sem, mid_sem, cross_sem, near_sem, far_out_sem,
):
    rank = plan.rank
    z, x, col = lax.axis_index("dp"), lax.axis_index("row"), lax.axis_index("col")
    core, y = lax.rem(col, 2), col // 2
    peers = {
        "pair": [(col, {"col": y * 2 + 1 - core}, 1 - core)],
        "far": [], "dp": [], "row": [],
    }
    for d in range(1, plan.n_far):
        t = lax.rem(y + d, plan.n_far)
        peers["far"].append((d, {"col": t * 2 + core}, t))
    for d in range(1, plan.n_dp):
        t = lax.rem(z + d, plan.n_dp)
        peers["dp"].append((d, {"dp": t}, t))
    for d in range(1, plan.n_row):
        t = lax.rem(x + d, plan.n_row)
        peers["row"].append((d, {"row": t}, t))
    everyone = [p for name in ("pair", "far", "dp", "row") for p in peers[name]]

    def load(c):
        rows = pl.ds(pl.multiple_of(c * plan.p_rows, plan.p_rows), plan.p_rows)
        return (
            pltpu.make_async_copy(g_hbm.at[0, rows], g.at[0, rows], load_sem.at[0, c]),
            pltpu.make_async_copy(e_hbm.at[0, rows], e.at[rows], load_sem.at[1, c]),
        )

    @pl.loop(0, plan.p_chunks)
    def _(c):
        for copy in load(c):
            copy.start()

    barrier = pltpu.get_barrier_semaphore()
    for _, device, _ in everyone:
        pl.semaphore_signal(barrier, inc=1, device_id=device, device_id_type=MESH)
    pl.semaphore_wait(barrier, len(everyone))

    @pl.loop(0, plan.q_chunks)
    def _(c):
        rows = pl.ds(pl.multiple_of(c * plan.q_cols, plan.q_cols), plan.q_cols)
        high, low = split_bf16(q_in[rows, :])
        factor[rows, :rank] = high
        factor[rows, rank:] = low

    def remote(src, dst, sems, index, device):
        return pltpu.make_async_remote_copy(
            src_ref=src, dst_ref=dst,
            send_sem=sems.at[(0,) + index], recv_sem=sems.at[(1,) + index],
            device_id=device, device_id_type=MESH,
        )

    def p_slice(c, *parts):
        start, size = c * plan.p_rows, plan.p_rows
        for part, width in zip(parts, (plan.p_pair, plan.p_far, plan.p_dp)):
            start, size = start + part * width, width
        return pl.ds(pl.multiple_of(start, 8), size)

    def small(c, size):
        return pl.ds(pl.multiple_of(c * size, 8), size)

    def pair_rs(c):
        return [
            remote(p_sum.at[p_slice(c, t)], pair_in.at[small(c, plan.p_pair)], pair_sem, (c,), dev)
            for _, dev, t in peers["pair"]
        ]

    def far_rs(c):
        return [
            remote(p_sum.at[p_slice(c, core, t)], far_in.at[d - 1, small(c, plan.p_far)], far_sem, (c, d - 1), dev)
            for d, dev, t in peers["far"]
        ]

    def pdp_rs(c):
        return [
            remote(p_sum.at[p_slice(c, core, y, t)], p_dp_in.at[d - 1, small(c, plan.p_dp)], pdp_sem, (c, d - 1), dev)
            for d, dev, t in peers["dp"]
        ]

    def pdp_ag(c):
        mine = p_slice(c, core, y, z)
        return [remote(p_all.at[mine], p_all.at[mine], pdp2_sem, (c, d - 1), dev) for d, dev, _ in peers["dp"]]

    def far_ag(c):
        mine = p_slice(c, core, y)
        return [remote(p_all.at[mine], p_all.at[mine], far2_sem, (c, d - 1), dev) for d, dev, _ in peers["far"]]

    def pair_ag(c):
        mine = p_slice(c, core)
        return [remote(p_all.at[mine], p_all.at[mine], pair2_sem, (c,), dev) for _, dev, _ in peers["pair"]]

    def q_slice(part):
        return pl.ds(pl.multiple_of(part * plan.q_row, 8), plan.q_row)

    side = z // 2
    inner = (z == 1) | (z == 2)
    near, far_half = pl.ds(pl.multiple_of(side * plan.q_half, 8), plan.q_half), pl.ds(
        pl.multiple_of((1 - side) * plan.q_half, 8), plan.q_half
    )
    opposite = {"dp": 3 - z}
    towards = {"dp": jnp.where(side == 0, 1, 2)}
    outwards = {"dp": jnp.where(side == 0, 0, 3)}
    above, below = {"dp": jnp.minimum(z + 1, 3)}, {"dp": jnp.maximum(z - 1, 0)}

    def row_rs(c):
        return [
            remote(q_sum.at[c, q_slice(t)], row_in.at[d - 1, c], row_sem, (c, d - 1), dev)
            for d, dev, t in peers["row"]
        ]

    def row_ag(c):
        mine = q_slice(x)
        return [remote(q_all.at[c, mine], q_all.at[c, mine], row2_sem, (c, d - 1), dev) for d, dev, _ in peers["row"]]

    def up(c):
        return remote(up_out.at[c], up_in.at[c], up_sem, (c,), above)

    def down(c):
        return remote(down_out.at[c], down_in.at[c], down_sem, (c,), below)

    def end(c):
        return remote(q_sum.at[c], end_in.at[c], end_sem, (c,), towards)

    def middle(c):
        return remote(q_sum.at[c, far_half], mid_in.at[c], mid_sem, (c,), opposite)

    def row_swap(c):
        return [
            remote(q_sum.at[c, near], row_in.at[d - 1, c], row_sem, (c, d - 1), dev)
            for d, dev, _ in peers["row"]
        ]

    def cross(c):
        return remote(q_all.at[c, near], q_all.at[c, near], cross_sem, (c,), opposite)

    def near_out(c):
        return remote(q_all.at[c, near], q_all.at[c, near], near_sem, (c,), outwards)

    def far_out(c):
        return remote(q_all.at[c, far_half], q_all.at[c, far_half], far_out_sem, (c,), outwards)

    def cross_in(c):
        return remote(q_all.at[c, far_half], q_all.at[c, far_half], cross_sem, (c,), opposite)

    def start(copies):
        for copy in copies:
            copy.start()

    def wait(copies):
        for copy in copies:
            copy.wait()

    scale = 1.0 / plan.n_dp

    def stage(t, lag, index, chunks, body):
        c = t - lag * index
        @pl.when((c >= 0) & (c < chunks))
        def _():
            body(c)

    def gram_copies():
        return [
            remote(gram, gram_in.at[d - 1], gram_sem, (d - 1,), dev) for d, dev, _ in peers["row"]
        ]

    lanes = lax.broadcasted_iota(jnp.int32, (rank, rank), 1)
    sublanes = lax.broadcasted_iota(jnp.int32, (rank, rank), 0)
    last_pivot = USE_Q - STEPS_P_HAT
    per_step = -(-(rank // 2) // (last_pivot - 2))
    quarter = rank // 8
    hat_chunks = -(-plan.p_chunks // STEPS_P_HAT)

    def eliminate(j, low):
        pair = [work[pl.ds(j + k, 1), :] for k in range(2)]
        unit = [inverse[pl.ds(j + k, 1), :] for k in range(2)]
        square = work[low:, :]
        line, down_rows = lanes[low:], sublanes[low:, :1]

        def entry(row, k):
            return jnp.sum(jnp.where(lanes[:1] == j + k, row, 0.0), axis=1, keepdims=True)

        def column(k):
            return jnp.sum(jnp.where(line == j + k, square, 0.0), axis=1, keepdims=True)

        first, second = column(0), column(1)
        over = entry(pair[0], 1)
        pivot = 1.0 / entry(pair[0], 0)
        ratio = entry(pair[1], 0) * pivot
        next_pivot = 1.0 / (entry(pair[1], 1) - ratio * over)
        pair[1] = pair[1] - ratio * pair[0]
        unit[1] = unit[1] - ratio * unit[0]
        first = jnp.where(down_rows > j, first * pivot, 0.0)
        second = jnp.where(down_rows > j + 1, (second - first * over) * next_pivot, 0.0)
        work[low:, :] = square - first * pair[0] - second * pair[1]
        inverse[low:, :] = inverse[low:, :] - first * unit[0] - second * unit[1]

    @pl.loop(0, ITERS)
    def _(step):
        def p_make(c):
            @pl.when(step == 0)
            def _():
                wait(load(c))
            rows = p_slice(c)
            both = dot(g[0, rows, :], factor[...], 1, 0) + dot(e[rows, :], factor[...], 1, 0)
            p_sum[rows, :] = both[:, :rank] + both[:, rank:]
            start(pair_rs(c))

        def p_pair(c):
            wait(pair_rs(c))
            rows = p_slice(c, core)
            p_sum[rows, :] = p_sum[rows, :] + pair_in[small(c, plan.p_pair), :]
            start(far_rs(c))

        def p_far(c):
            wait(far_rs(c))
            rows = p_slice(c, core, y)
            total = p_sum[rows, :]
            for d, _, _ in peers["far"]:
                total = total + far_in[d - 1, small(c, plan.p_far), :]
            p_sum[rows, :] = total
            start(pdp_rs(c))

        def p_dp(c):
            wait(pdp_rs(c))
            rows = p_slice(c, core, y, z)
            total = p_sum[rows, :]
            for d, _, _ in peers["dp"]:
                total = total + p_dp_in[d - 1, small(c, plan.p_dp), :]
            p_all[rows, :] = total * scale
            start(pdp_ag(c))

        def p_far2(c):
            wait(pdp_ag(c))
            start(far_ag(c))

        def p_pair2(c):
            wait(far_ag(c))
            start(pair_ag(c))

        def p_use(c):
            wait(pair_ag(c))
            for part in range(plan.p_rows // 128):
                rows = pl.ds(pl.multiple_of(c * plan.p_rows + part * 128, 128), 128)
                high, low = split_bf16(jnp.transpose(p_all[rows, :]))
                p_t[:rank, rows] = high
                p_t[rank:, rows] = low

        @pl.loop(0, plan.p_chunks + 6 * LAG_P)
        def _(t):
            for index, body in enumerate((p_make, p_pair, p_far, p_dp, p_far2, p_pair2, p_use)):
                stage(t, LAG_P, index, plan.p_chunks, body)

        square = dot(p_t[...], p_t[...], 1, 1)
        gram[...] = square[:rank, :rank] + square[:rank, rank:] + square[rank:, :rank] + square[rank:, rank:]
        start(gram_copies())

        def even(c, condition=True):
            return (lax.rem(c, 3) != 0) & condition

        def odd(c, condition=True):
            return (lax.rem(c, 3) == 0) & condition

        def q_make(c):
            cols = pl.ds(pl.multiple_of(c * plan.q_cols, plan.q_cols), plan.q_cols)
            both = dot(p_t[...], g[0, :, cols], 1, 0) + dot(p_t[...], e[:, cols], 1, 0)
            q_sum[c] = both[:rank] + both[rank:]

            @pl.when(even(c))
            def _():
                start(row_rs(c))

            @pl.when(odd(c, jnp.logical_not(inner)))
            def _():
                end(c).start()

        def q_first(c):
            @pl.when(even(c))
            def _():
                wait(row_rs(c))
                mine = q_slice(x)
                total = q_sum[c, mine, :]
                for d, _, _ in peers["row"]:
                    total = total + row_in[d - 1, c]
                q_sum[c, mine, :] = total

                @pl.when(z == 0)
                def _():
                    up_out[c] = total
                    up(c).start()

                @pl.when(z == 3)
                def _():
                    down_out[c] = total
                    down(c).start()

            @pl.when(odd(c, inner))
            def _():
                end(c).wait_recv()
                q_sum[c] = q_sum[c] + end_in[c]
                middle(c).start()

        def q_up(c):
            @pl.when(even(c, z > 0))
            def _():
                up(c).wait_recv()
                up_out[c] = up_in[c] + q_sum[c, q_slice(x), :]

                @pl.when(z < 3)
                def _():
                    up(c).start()

        def q_down(c):
            @pl.when(even(c, z < 3))
            def _():
                down(c).wait_recv()

                @pl.when(z > 0)
                def _():
                    down_out[c] = down_in[c] + q_sum[c, q_slice(x), :]
                    down(c).start()

        def q_second(c):
            @pl.when(odd(c, inner))
            def _():
                middle(c).wait_recv()
                q_sum[c, near, :] = q_sum[c, near, :] + mid_in[c]
                start(row_swap(c))

        def q_third(c):
            @pl.when(odd(c, inner))
            def _():
                wait(row_swap(c))
                total = q_sum[c, near, :]
                for d, _, _ in peers["row"]:
                    total = total + row_in[d - 1, c]
                q_all[c, near, :] = total * scale
                near_out(c).start()
                cross(c).start()

        def q_fourth(c):
            @pl.when(even(c))
            def _():
                mine = q_slice(x)

                @pl.when(z == 0)
                def _():
                    q_all[c, mine, :] = (q_sum[c, mine, :] + down_in[c]) * scale

                @pl.when(inner)
                def _():
                    q_all[c, mine, :] = (up_out[c] + down_in[c]) * scale

                @pl.when(z == 3)
                def _():
                    q_all[c, mine, :] = up_out[c] * scale

                start(row_ag(c))

            @pl.when(odd(c, inner))
            def _():
                cross_in(c).wait_recv()
                far_out(c).start()

            @pl.when(odd(c, jnp.logical_not(inner)))
            def _():
                near_out(c).wait_recv()

        def q_fifth(c):
            @pl.when(even(c))
            def _():
                wait(row_ag(c))

                @pl.when(z < 3)
                def _():
                    up(c).wait_send()

                @pl.when(z > 0)
                def _():
                    down(c).wait_send()

            @pl.when(odd(c, inner))
            def _():
                middle(c).wait_send()
                near_out(c).wait_send()
                cross(c).wait_send()
                far_out(c).wait_send()

            @pl.when(odd(c, jnp.logical_not(inner)))
            def _():
                end(c).wait_send()
                far_out(c).wait_recv()

        def q_use(c):
            rows = pl.ds(pl.multiple_of(c * plan.q_cols, plan.q_cols), plan.q_cols)
            value = lax.dot_general(
                jnp.transpose(q_all[c]), inverse[...], (((1,), (1,)), ((), ())),
                precision=lax.Precision.HIGHEST, preferred_element_type=jnp.float32,
            )
            q_out[rows, :] = value
            high, low = split_bf16(value)
            factor[rows, :rank] = high
            factor[rows, rank:] = low

            @pl.when(step == ITERS - 1)
            def _():
                right = factor[rows, :]

                @pl.loop(0, plan.rows // RESIDUAL_ROWS)
                def _(block):
                    part = pl.ds(pl.multiple_of(block * RESIDUAL_ROWS, RESIDUAL_ROWS), RESIDUAL_ROWS)
                    approx = dot(left[0, part, :], right, 1, 1) + dot(left[1, part, :], right, 1, 1)
                    comp = g[0, part, rows].astype(jnp.float32) + e[part, rows].astype(jnp.float32)
                    g[0, part, rows] = (comp - approx).astype(jnp.bfloat16)

        def p_hat(c):
            rows = p_slice(c)
            value = lax.dot_general(
                p_all[rows, :], inverse[...], (((1,), (1,)), ((), ())),
                precision=lax.Precision.HIGHEST, preferred_element_type=jnp.float32,
            )
            high, low = split_bf16(value)
            left[0, rows, :rank] = high
            left[0, rows, rank:] = low
            left[1, rows, :rank] = low
            left[1, rows, rank:] = high

        @pl.loop(0, plan.q_chunks + max(USE_Q, 5 * LAG_Q))
        def _(t):
            stage(t, LAG_Q, 0, plan.q_chunks, q_make)
            stage(t, LAG_Q, 1, plan.q_chunks, q_first)
            stage(t, LAG_Q, 1 + z, plan.q_chunks, q_up)
            stage(t, LAG_Q, 4 - z, plan.q_chunks, q_down)
            stage(t, LAG_Q, 2, plan.q_chunks, q_second)
            stage(t, LAG_Q, 3, plan.q_chunks, q_third)
            stage(t, LAG_Q, 4, plan.q_chunks, q_fourth)
            stage(t, LAG_Q, 5, plan.q_chunks, q_fifth)

            @pl.when(t == 2)
            def _():
                wait(gram_copies())
                total = gram[...]
                for d, _, _ in peers["row"]:
                    total = total + gram_in[d - 1]
                work[...] = total
                inverse[...] = jnp.where(lanes == sublanes, 1.0, 0.0)

            @pl.when((t >= 2) & (t < last_pivot))
            def _():
                first = (t - 2) * per_step

                for part in range(4):
                    begin = jnp.maximum(first, part * quarter)
                    end_ = jnp.minimum(first + per_step, (part + 1) * quarter)

                    @pl.loop(begin, jnp.maximum(begin, end_))
                    def _(j, part=part):
                        eliminate(2 * j, 2 * part * quarter)

            @pl.when(t == last_pivot)
            def _():
                diagonal = jnp.sum(jnp.where(lanes == sublanes, work[...], 0.0), axis=1, keepdims=True)
                inverse[...] = inverse[...] / jnp.sqrt(diagonal)

            @pl.when((step == ITERS - 1) & (t >= last_pivot) & (t < USE_Q))
            def _():
                first = (t - last_pivot) * hat_chunks

                @pl.loop(first, jnp.minimum(first + hat_chunks, plan.p_chunks))
                def _(c):
                    p_hat(c)

            stage(t, USE_Q, 1, plan.q_chunks, q_use)


def store_kernel(plan, residual, q_mat, new_error, q_factor, sem, q_sem):
    def blocks(c):
        rows = pl.ds(pl.multiple_of(c * plan.p_rows, plan.p_rows), plan.p_rows)
        return pltpu.make_async_copy(residual.at[0, rows], new_error.at[0, rows], sem.at[c])

    last = pltpu.make_async_copy(q_mat, q_factor, q_sem)
    for c in range(plan.p_chunks):
        blocks(c).start()
    last.start()
    for c in range(plan.p_chunks):
        blocks(c).wait()
    last.wait()


def fused(plan, grad, error, q_init):
    rows, cols, rank = plan.rows, plan.cols, plan.rank
    pc, qc = plan.p_chunks, plan.q_chunks
    f32, bf16 = jnp.float32, jnp.bfloat16
    dma = pltpu.SemaphoreType.DMA
    dp, row, far = plan.n_dp - 1, plan.n_row - 1, plan.n_far - 1
    whole = pl.BlockSpec(memory_space=pltpu.VMEM)
    part = pltpu.VMEM((qc, plan.q_row, plan.q_cols), f32)
    residual, q_mat = pl.pallas_call(
        functools.partial(iterate_kernel, plan),
        out_shape=[pltpu.VMEM((1, rows, cols), bf16), pltpu.VMEM((cols, rank), f32)],
        in_specs=[pl.BlockSpec(memory_space=pl.ANY)] * 2 + [whole],
        out_specs=[whole] * 2,
        scratch_shapes=[
            pltpu.VMEM((rows, cols), bf16),
            pltpu.VMEM((cols, 2 * rank), bf16), pltpu.VMEM((2, rows, 2 * rank), bf16),
            pltpu.VMEM((2 * rank, rows), bf16),
            pltpu.VMEM((rows, rank), f32), pltpu.VMEM((rows, rank), f32),
            pltpu.VMEM((qc, rank, plan.q_cols), f32), pltpu.VMEM((qc, rank, plan.q_cols), f32),
            pltpu.VMEM((pc * plan.p_pair, rank), f32),
            pltpu.VMEM((far, pc * plan.p_far, rank), f32),
            pltpu.VMEM((dp, pc * plan.p_dp, rank), f32),
            pltpu.VMEM((row, qc, max(plan.q_row, plan.q_half), plan.q_cols), f32),
            part, part, part, part,
            pltpu.VMEM((qc, rank, plan.q_cols), f32),
            pltpu.VMEM((qc, plan.q_half, plan.q_cols), f32),
            pltpu.VMEM((rank, rank), f32), pltpu.VMEM((row, rank, rank), f32),
            pltpu.VMEM((rank, rank), f32), pltpu.VMEM((rank, rank), f32),
            dma((2, pc)), dma((2, row)), dma((2, pc)), dma((2, pc, far)),
            dma((2, pc, dp)), dma((2, pc, dp)), dma((2, pc, far)), dma((2, pc)),
            dma((2, qc, row)), dma((2, qc, row)), dma((2, qc)), dma((2, qc)),
            dma((2, qc)), dma((2, qc)), dma((2, qc)), dma((2, qc)), dma((2, qc)),
        ],
        compiler_params=pltpu.CompilerParams(
            collective_id=0, has_side_effects=True, vmem_limit_bytes=VMEM_BYTES
        ),
        name="iterate",
    )(grad, error, q_init)
    return pl.pallas_call(
        functools.partial(store_kernel, plan),
        out_shape=[
            jax.ShapeDtypeStruct((1, rows, cols), bf16), jax.ShapeDtypeStruct((cols, rank), f32)
        ],
        in_specs=[whole] * 2,
        out_specs=[pl.BlockSpec(memory_space=pl.ANY)] * 2,
        scratch_shapes=[dma((pc,)), dma(())],
        compiler_params=pltpu.CompilerParams(vmem_limit_bytes=4 << 20),
        name="store",
    )(residual, q_mat)


def solution(mesh):
    in_specs = (P("dp", "row", "col"), P("dp", "row", "col"), P("col", None))
    out_specs = (P("dp", "row", "col"), P("col", None))
    sizes = dict(mesh.shape)

    def step(grad, error, q_init):
        plan = Plan(sizes, grad.shape[1], grad.shape[2], q_init.shape[1])
        if plan.fits(sizes):
            return tuple(fused(plan, grad, error, q_init))
        return shards(grad, error, q_init)

    return jax.shard_map(step, mesh=mesh, in_specs=in_specs, out_specs=out_specs, check_vma=False)
```

```python
import functools

import jax
import jax.numpy as jnp
from jax import lax
from jax.experimental import pallas as pl
from jax.experimental.pallas import tpu as pltpu
from jax.sharding import PartitionSpec as P

ITERS = 2


def power_of_two(n):
    return n & (n - 1) == 0


def exchange(value, axis, bit):
    n = lax.axis_size(axis)
    return lax.ppermute(value, axis, [(i, i ^ bit) for i in range(n)])


def bits_of(axes):
    steps = []
    for axis in axes:
        bit = 1
        while bit < lax.axis_size(axis):
            steps.append((axis, bit))
            bit *= 2
    return steps


def upper(axis, bit):
    return lax.rem(lax.axis_index(axis) // bit, 2)


def butterfly(values_axes):
    state = [(value, bits_of(axes)) for value, axes in values_axes]
    values = [value for value, _ in state]
    depth = len(state[0][1])
    for level in range(depth):
        for k, (_, steps) in enumerate(state):
            axis, bit = steps[level]
            half = values[k].shape[0] // 2
            side = upper(axis, bit)
            keep = lax.dynamic_slice_in_dim(values[k], side * half, half, 0)
            give = lax.dynamic_slice_in_dim(values[k], (1 - side) * half, half, 0)
            values[k] = keep + exchange(give, axis, bit)
    for level in reversed(range(depth)):
        for k, (_, steps) in enumerate(state):
            axis, bit = steps[level]
            first = upper(axis, bit) == 0
            mine = values[k]
            other = exchange(mine, axis, bit)
            values[k] = jnp.concatenate(
                [jnp.where(first, mine, other), jnp.where(first, other, mine)], axis=0
            )
    return values


def reduce_over(value, axis_a, axis_b):
    sizes = lax.axis_size(axis_a), lax.axis_size(axis_b)
    rows = value.shape[0]
    if not all(map(power_of_two, sizes)) or rows % (2 * sizes[0] * sizes[1]):
        return lax.psum(value, (axis_a, axis_b))
    half = rows // 2
    parts = butterfly(
        [(value[:half], (axis_a, axis_b)), (value[half:], (axis_b, axis_a))]
    )
    return jnp.concatenate(parts, axis=0)


def reduce_small(value, axis):
    if not power_of_two(lax.axis_size(axis)):
        return lax.psum(value, axis)
    for name, bit in bits_of((axis,)):
        value = value + exchange(value, name, bit)
    return value


def split(value):
    high = lax.reduce_precision(value, exponent_bits=8, mantissa_bits=7)
    return high.astype(jnp.bfloat16), (value - high).astype(jnp.bfloat16)


def product(high, low, factor, side):
    rank = factor.shape[1]
    both = jnp.concatenate(split(factor), axis=1)
    dims = (((side,), (0,)), ((), ()))
    total = lax.dot_general(high, both, dims, preferred_element_type=jnp.float32)
    total = total + lax.dot_general(low, both, dims, preferred_element_type=jnp.float32)
    return total[:, :rank] + total[:, rank:]


def exact_dot(a, b, dims):
    return lax.dot_general(
        a, b, (dims, ((), ())), precision=lax.Precision.HIGHEST,
        preferred_element_type=jnp.float32,
    )


def shards(grad, error, q_init):
    comp = grad[0].astype(jnp.float32) + error[0].astype(jnp.float32)
    high, low = lax.optimization_barrier(split(comp))
    scale = 1.0 / lax.axis_size("dp")
    q_mat = q_init
    p_hat = None
    eye = jnp.eye(q_init.shape[1], dtype=jnp.float32)
    for step in range(ITERS):
        p_mat = reduce_over(product(high, low, q_mat, 1), "col", "dp") * scale
        gram = reduce_small(exact_dot(p_mat, p_mat, ((0,), (0,))), "row")
        term = reduce_over(product(high, low, p_mat, 0), "row", "dp") * scale
        lower = jnp.linalg.cholesky(gram)
        inverse = jax.scipy.linalg.solve_triangular(lower, eye, lower=True)
        q_mat = exact_dot(term, inverse, ((1,), (1,)))
        p_hat = exact_dot(p_mat, inverse, ((1,), (1,)))
    p_high, p_low = split(p_hat)
    q_high, q_low = split(q_mat)
    left = jnp.concatenate([p_high, p_high, p_low], axis=1)
    right = jnp.concatenate([q_high, q_low, q_high], axis=1)
    approx = lax.dot_general(
        left, right, (((1,), (1,)), ((), ())), preferred_element_type=jnp.float32
    )
    comp = grad[0].astype(jnp.float32) + error[0].astype(jnp.float32)
    new_error = (comp - approx).astype(jnp.bfloat16)[None]
    return (new_error, q_mat)


MESH = pl.DeviceIdType.MESH
CHUNK_ROWS = 256
CHUNK_COLS = 256
LAG_P = 3
LAG_Q = 2
USE_Q = 10
STEPS_P_HAT = 2
RESIDUAL_ROWS = 2048
VMEM_BYTES = 45 << 20


def split_bf16(value):
    high = value.astype(jnp.bfloat16)
    low = (value - high.astype(jnp.float32)).astype(jnp.bfloat16)
    return high, low


def dot(a, b, side_a, side_b):
    return lax.dot_general(
        a, b, (((side_a,), (side_b,)), ((), ())), preferred_element_type=jnp.float32
    )


class Plan:
    def __init__(self, mesh, rows, cols, rank):
        self.rows, self.cols, self.rank = rows, cols, rank
        self.n_dp, self.n_row = mesh["dp"], mesh["row"]
        self.n_pair = 2
        self.n_far = mesh["col"] // 2
        self.p_rows, self.q_cols = CHUNK_ROWS, CHUNK_COLS
        self.p_chunks, self.q_chunks = rows // self.p_rows, cols // self.q_cols
        self.p_pair = self.p_rows // self.n_pair
        self.p_far = self.p_pair // max(self.n_far, 1)
        self.p_dp = self.p_far // self.n_dp
        self.q_row = rank // self.n_row
        self.q_half = rank // 2

    def fits(self, mesh):
        return (
            mesh["col"] % 2 == 0
            and self.n_dp == 4
            and self.n_far > 1
            and self.rank == 128
            and self.rows % self.p_rows == 0
            and self.cols % self.q_cols == 0
            and self.p_dp % 8 == 0
            and self.q_row % 8 == 0
            and self.n_row == 2
            and self.rows % RESIDUAL_ROWS == 0
            and self.p_far * self.n_far * self.n_pair == self.p_rows
            and self.p_dp * self.n_dp == self.p_far
            and self.q_row * self.n_row == self.rank
            and self.rows * self.cols * 4 <= 30 << 20
        )


def iterate_kernel(
    plan, g_hbm, e_hbm, q_in,
    g, q_out,
    e, factor, left, p_t, p_sum, p_all, q_sum, q_all,
    pair_in, far_in, p_dp_in, row_in, up_in, up_out, down_in, down_out, end_in, mid_in,
    gram, gram_in, work, inverse,
    load_sem, gram_sem, pair_sem, far_sem, pdp_sem, pdp2_sem, far2_sem, pair2_sem,
    row_sem, row2_sem, up_sem, down_sem, end_sem, mid_sem, cross_sem, near_sem, far_out_sem,
):
    rank = plan.rank
    z, x, col = lax.axis_index("dp"), lax.axis_index("row"), lax.axis_index("col")
    core, y = lax.rem(col, 2), col // 2
    peers = {
        "pair": [(col, {"col": y * 2 + 1 - core}, 1 - core)],
        "far": [], "dp": [], "row": [],
    }
    for d in range(1, plan.n_far):
        t = lax.rem(y + d, plan.n_far)
        peers["far"].append((d, {"col": t * 2 + core}, t))
    for d in range(1, plan.n_dp):
        t = lax.rem(z + d, plan.n_dp)
        peers["dp"].append((d, {"dp": t}, t))
    for d in range(1, plan.n_row):
        t = lax.rem(x + d, plan.n_row)
        peers["row"].append((d, {"row": t}, t))
    everyone = [p for name in ("pair", "far", "dp", "row") for p in peers[name]]

    def load(c):
        rows = pl.ds(pl.multiple_of(c * plan.p_rows, plan.p_rows), plan.p_rows)
        return (
            pltpu.make_async_copy(g_hbm.at[0, rows], g.at[0, rows], load_sem.at[0, c]),
            pltpu.make_async_copy(e_hbm.at[0, rows], e.at[rows], load_sem.at[1, c]),
        )

    @pl.loop(0, plan.p_chunks)
    def _(c):
        for copy in load(c):
            copy.start()

    barrier = pltpu.get_barrier_semaphore()
    for _, device, _ in everyone:
        pl.semaphore_signal(barrier, inc=1, device_id=device, device_id_type=MESH)
    pl.semaphore_wait(barrier, len(everyone))

    @pl.loop(0, plan.q_chunks)
    def _(c):
        rows = pl.ds(pl.multiple_of(c * plan.q_cols, plan.q_cols), plan.q_cols)
        high, low = split_bf16(q_in[rows, :])
        factor[rows, :rank] = high
        factor[rows, rank:] = low

    def remote(src, dst, sems, index, device):
        return pltpu.make_async_remote_copy(
            src_ref=src, dst_ref=dst,
            send_sem=sems.at[(0,) + index], recv_sem=sems.at[(1,) + index],
            device_id=device, device_id_type=MESH,
        )

    def p_slice(c, *parts):
        start, size = c * plan.p_rows, plan.p_rows
        for part, width in zip(parts, (plan.p_pair, plan.p_far, plan.p_dp)):
            start, size = start + part * width, width
        return pl.ds(pl.multiple_of(start, 8), size)

    def small(c, size):
        return pl.ds(pl.multiple_of(c * size, 8), size)

    def pair_rs(c):
        return [
            remote(p_sum.at[p_slice(c, t)], pair_in.at[small(c, plan.p_pair)], pair_sem, (c,), dev)
            for _, dev, t in peers["pair"]
        ]

    def far_rs(c):
        return [
            remote(p_sum.at[p_slice(c, core, t)], far_in.at[d - 1, small(c, plan.p_far)], far_sem, (c, d - 1), dev)
            for d, dev, t in peers["far"]
        ]

    def pdp_rs(c):
        return [
            remote(p_sum.at[p_slice(c, core, y, t)], p_dp_in.at[d - 1, small(c, plan.p_dp)], pdp_sem, (c, d - 1), dev)
            for d, dev, t in peers["dp"]
        ]

    def pdp_ag(c):
        mine = p_slice(c, core, y, z)
        return [remote(p_all.at[mine], p_all.at[mine], pdp2_sem, (c, d - 1), dev) for d, dev, _ in peers["dp"]]

    def far_ag(c):
        mine = p_slice(c, core, y)
        return [remote(p_all.at[mine], p_all.at[mine], far2_sem, (c, d - 1), dev) for d, dev, _ in peers["far"]]

    def pair_ag(c):
        mine = p_slice(c, core)
        return [remote(p_all.at[mine], p_all.at[mine], pair2_sem, (c,), dev) for _, dev, _ in peers["pair"]]

    def q_slice(part):
        return pl.ds(pl.multiple_of(part * plan.q_row, 8), plan.q_row)

    side = z // 2
    inner = (z == 1) | (z == 2)
    near, far_half = pl.ds(pl.multiple_of(side * plan.q_half, 8), plan.q_half), pl.ds(
        pl.multiple_of((1 - side) * plan.q_half, 8), plan.q_half
    )
    opposite = {"dp": 3 - z}
    towards = {"dp": jnp.where(side == 0, 1, 2)}
    outwards = {"dp": jnp.where(side == 0, 0, 3)}
    above, below = {"dp": jnp.minimum(z + 1, 3)}, {"dp": jnp.maximum(z - 1, 0)}

    def row_rs(c):
        return [
            remote(q_sum.at[c, q_slice(t)], row_in.at[d - 1, c], row_sem, (c, d - 1), dev)
            for d, dev, t in peers["row"]
        ]

    def row_ag(c):
        mine = q_slice(x)
        return [remote(q_all.at[c, mine], q_all.at[c, mine], row2_sem, (c, d - 1), dev) for d, dev, _ in peers["row"]]

    def up(c):
        return remote(up_out.at[c], up_in.at[c], up_sem, (c,), above)

    def down(c):
        return remote(down_out.at[c], down_in.at[c], down_sem, (c,), below)

    def end(c):
        return remote(q_sum.at[c], end_in.at[c], end_sem, (c,), towards)

    def middle(c):
        return remote(q_sum.at[c, far_half], mid_in.at[c], mid_sem, (c,), opposite)

    def row_swap(c):
        return [
            remote(q_sum.at[c, near], row_in.at[d - 1, c], row_sem, (c, d - 1), dev)
            for d, dev, _ in peers["row"]
        ]

    def cross(c):
        return remote(q_all.at[c, near], q_all.at[c, near], cross_sem, (c,), opposite)

    def near_out(c):
        return remote(q_all.at[c, near], q_all.at[c, near], near_sem, (c,), outwards)

    def far_out(c):
        return remote(q_all.at[c, far_half], q_all.at[c, far_half], far_out_sem, (c,), outwards)

    def cross_in(c):
        return remote(q_all.at[c, far_half], q_all.at[c, far_half], cross_sem, (c,), opposite)

    def start(copies):
        for copy in copies:
            copy.start()

    def wait(copies):
        for copy in copies:
            copy.wait()

    scale = 1.0 / plan.n_dp

    def stage(t, lag, index, chunks, body):
        c = t - lag * index
        @pl.when((c >= 0) & (c < chunks))
        def _():
            body(c)

    def gram_copies():
        return [
            remote(gram, gram_in.at[d - 1], gram_sem, (d - 1,), dev) for d, dev, _ in peers["row"]
        ]

    lanes = lax.broadcasted_iota(jnp.int32, (rank, rank), 1)
    sublanes = lax.broadcasted_iota(jnp.int32, (rank, rank), 0)
    last_pivot = USE_Q - STEPS_P_HAT
    per_step = -(-(rank // 2) // (last_pivot - 2))
    quarter = rank // 8
    hat_chunks = -(-plan.p_chunks // STEPS_P_HAT)

    def eliminate(j, low):
        pair = [work[pl.ds(j + k, 1), :] for k in range(2)]
        unit = [inverse[pl.ds(j + k, 1), :] for k in range(2)]
        square = work[low:, :]
        line, down_rows = lanes[low:], sublanes[low:, :1]

        def entry(row, k):
            return jnp.sum(jnp.where(lanes[:1] == j + k, row, 0.0), axis=1, keepdims=True)

        def column(k):
            return jnp.sum(jnp.where(line == j + k, square, 0.0), axis=1, keepdims=True)

        first, second = column(0), column(1)
        over = entry(pair[0], 1)
        pivot = 1.0 / entry(pair[0], 0)
        ratio = entry(pair[1], 0) * pivot
        next_pivot = 1.0 / (entry(pair[1], 1) - ratio * over)
        pair[1] = pair[1] - ratio * pair[0]
        unit[1] = unit[1] - ratio * unit[0]
        first = jnp.where(down_rows > j, first * pivot, 0.0)
        second = jnp.where(down_rows > j + 1, (second - first * over) * next_pivot, 0.0)
        work[low:, :] = square - first * pair[0] - second * pair[1]
        inverse[low:, :] = inverse[low:, :] - first * unit[0] - second * unit[1]

    @pl.loop(0, ITERS)
    def _(step):
        def p_make(c):
            @pl.when(step == 0)
            def _():
                wait(load(c))
            rows = p_slice(c)
            both = dot(g[0, rows, :], factor[...], 1, 0) + dot(e[rows, :], factor[...], 1, 0)
            p_sum[rows, :] = both[:, :rank] + both[:, rank:]
            start(pair_rs(c))

        def p_pair(c):
            wait(pair_rs(c))
            rows = p_slice(c, core)
            p_sum[rows, :] = p_sum[rows, :] + pair_in[small(c, plan.p_pair), :]
            start(far_rs(c))

        def p_far(c):
            wait(far_rs(c))
            rows = p_slice(c, core, y)
            total = p_sum[rows, :]
            for d, _, _ in peers["far"]:
                total = total + far_in[d - 1, small(c, plan.p_far), :]
            p_sum[rows, :] = total
            start(pdp_rs(c))

        def p_dp(c):
            wait(pdp_rs(c))
            rows = p_slice(c, core, y, z)
            total = p_sum[rows, :]
            for d, _, _ in peers["dp"]:
                total = total + p_dp_in[d - 1, small(c, plan.p_dp), :]
            p_all[rows, :] = total * scale
            start(pdp_ag(c))

        def p_far2(c):
            wait(pdp_ag(c))
            start(far_ag(c))

        def p_pair2(c):
            wait(far_ag(c))
            start(pair_ag(c))

        def p_use(c):
            wait(pair_ag(c))
            for part in range(plan.p_rows // 128):
                rows = pl.ds(pl.multiple_of(c * plan.p_rows + part * 128, 128), 128)
                high, low = split_bf16(jnp.transpose(p_all[rows, :]))
                p_t[:rank, rows] = high
                p_t[rank:, rows] = low

        @pl.loop(0, plan.p_chunks + 6 * LAG_P)
        def _(t):
            for index, body in enumerate((p_make, p_pair, p_far, p_dp, p_far2, p_pair2, p_use)):
                stage(t, LAG_P, index, plan.p_chunks, body)

        square = dot(p_t[...], p_t[...], 1, 1)
        gram[...] = square[:rank, :rank] + square[:rank, rank:] + square[rank:, :rank] + square[rank:, rank:]
        start(gram_copies())

        def even(c, condition=True):
            return (lax.rem(c, 3) != 0) & condition

        def odd(c, condition=True):
            return (lax.rem(c, 3) == 0) & condition

        def q_make(c):
            cols = pl.ds(pl.multiple_of(c * plan.q_cols, plan.q_cols), plan.q_cols)
            both = dot(p_t[...], g[0, :, cols], 1, 0) + dot(p_t[...], e[:, cols], 1, 0)
            q_sum[c] = both[:rank] + both[rank:]

            @pl.when(even(c))
            def _():
                start(row_rs(c))

            @pl.when(odd(c, jnp.logical_not(inner)))
            def _():
                end(c).start()

        def q_first(c):
            @pl.when(even(c))
            def _():
                wait(row_rs(c))
                mine = q_slice(x)
                total = q_sum[c, mine, :]
                for d, _, _ in peers["row"]:
                    total = total + row_in[d - 1, c]
                q_sum[c, mine, :] = total

                @pl.when(z == 0)
                def _():
                    up_out[c] = total
                    up(c).start()

                @pl.when(z == 3)
                def _():
                    down_out[c] = total
                    down(c).start()

            @pl.when(odd(c, inner))
            def _():
                end(c).wait_recv()
                q_sum[c] = q_sum[c] + end_in[c]
                middle(c).start()

        def q_up(c):
            @pl.when(even(c, z > 0))
            def _():
                up(c).wait_recv()
                up_out[c] = up_in[c] + q_sum[c, q_slice(x), :]

                @pl.when(z < 3)
                def _():
                    up(c).start()

        def q_down(c):
            @pl.when(even(c, z < 3))
            def _():
                down(c).wait_recv()

                @pl.when(z > 0)
                def _():
                    down_out[c] = down_in[c] + q_sum[c, q_slice(x), :]
                    down(c).start()

        def q_second(c):
            @pl.when(odd(c, inner))
            def _():
                middle(c).wait_recv()
                q_sum[c, near, :] = q_sum[c, near, :] + mid_in[c]
                start(row_swap(c))

        def q_third(c):
            @pl.when(odd(c, inner))
            def _():
                wait(row_swap(c))
                total = q_sum[c, near, :]
                for d, _, _ in peers["row"]:
                    total = total + row_in[d - 1, c]
                q_all[c, near, :] = total * scale
                near_out(c).start()
                cross(c).start()

        def q_fourth(c):
            @pl.when(even(c))
            def _():
                mine = q_slice(x)

                @pl.when(z == 0)
                def _():
                    q_all[c, mine, :] = (q_sum[c, mine, :] + down_in[c]) * scale

                @pl.when(inner)
                def _():
                    q_all[c, mine, :] = (up_out[c] + down_in[c]) * scale

                @pl.when(z == 3)
                def _():
                    q_all[c, mine, :] = up_out[c] * scale

                start(row_ag(c))

            @pl.when(odd(c, inner))
            def _():
                cross_in(c).wait_recv()
                far_out(c).start()

            @pl.when(odd(c, jnp.logical_not(inner)))
            def _():
                near_out(c).wait_recv()

        def q_fifth(c):
            @pl.when(even(c))
            def _():
                wait(row_ag(c))

                @pl.when(z < 3)
                def _():
                    up(c).wait_send()

                @pl.when(z > 0)
                def _():
                    down(c).wait_send()

            @pl.when(odd(c, inner))
            def _():
                middle(c).wait_send()
                near_out(c).wait_send()
                cross(c).wait_send()
                far_out(c).wait_send()

            @pl.when(odd(c, jnp.logical_not(inner)))
            def _():
                end(c).wait_send()
                far_out(c).wait_recv()

        def q_use(c):
            rows = pl.ds(pl.multiple_of(c * plan.q_cols, plan.q_cols), plan.q_cols)
            value = lax.dot_general(
                jnp.transpose(q_all[c]), inverse[...], (((1,), (1,)), ((), ())),
                precision=lax.Precision.HIGHEST, preferred_element_type=jnp.float32,
            )
            q_out[rows, :] = value
            high, low = split_bf16(value)
            factor[rows, :rank] = high
            factor[rows, rank:] = low

            @pl.when(step == ITERS - 1)
            def _():
                right = factor[rows, :]

                @pl.loop(0, plan.rows // RESIDUAL_ROWS)
                def _(block):
                    part = pl.ds(pl.multiple_of(block * RESIDUAL_ROWS, RESIDUAL_ROWS), RESIDUAL_ROWS)
                    approx = dot(left[0, part, :], right, 1, 1) + dot(left[1, part, :], right, 1, 1)
                    comp = g[0, part, rows].astype(jnp.float32) + e[part, rows].astype(jnp.float32)
                    g[0, part, rows] = (comp - approx).astype(jnp.bfloat16)

        def p_hat(c):
            rows = p_slice(c)
            value = lax.dot_general(
                p_all[rows, :], inverse[...], (((1,), (1,)), ((), ())),
                precision=lax.Precision.HIGHEST, preferred_element_type=jnp.float32,
            )
            high, low = split_bf16(value)
            left[0, rows, :rank] = high
            left[0, rows, rank:] = low
            left[1, rows, :rank] = low
            left[1, rows, rank:] = high

        @pl.loop(0, plan.q_chunks + max(USE_Q, 5 * LAG_Q))
        def _(t):
            stage(t, LAG_Q, 0, plan.q_chunks, q_make)
            stage(t, LAG_Q, 1, plan.q_chunks, q_first)
            stage(t, LAG_Q, 1 + z, plan.q_chunks, q_up)
            stage(t, LAG_Q, 4 - z, plan.q_chunks, q_down)
            stage(t, LAG_Q, 2, plan.q_chunks, q_second)
            stage(t, LAG_Q, 3, plan.q_chunks, q_third)
            stage(t, LAG_Q, 4, plan.q_chunks, q_fourth)
            stage(t, LAG_Q, 5, plan.q_chunks, q_fifth)

            @pl.when(t == 2)
            def _():
                wait(gram_copies())
                total = gram[...]
                for d, _, _ in peers["row"]:
                    total = total + gram_in[d - 1]
                work[...] = total
                inverse[...] = jnp.where(lanes == sublanes, 1.0, 0.0)

            @pl.when((t >= 2) & (t < last_pivot))
            def _():
                first = (t - 2) * per_step

                for part in range(4):
                    begin = jnp.maximum(first, part * quarter)
                    end_ = jnp.minimum(first + per_step, (part + 1) * quarter)

                    @pl.loop(begin, jnp.maximum(begin, end_))
                    def _(j, part=part):
                        eliminate(2 * j, 2 * part * quarter)

            @pl.when(t == last_pivot)
            def _():
                diagonal = jnp.sum(jnp.where(lanes == sublanes, work[...], 0.0), axis=1, keepdims=True)
                inverse[...] = inverse[...] / jnp.sqrt(diagonal)

            @pl.when((step == ITERS - 1) & (t >= last_pivot) & (t < USE_Q))
            def _():
                first = (t - last_pivot) * hat_chunks

                @pl.loop(first, jnp.minimum(first + hat_chunks, plan.p_chunks))
                def _(c):
                    p_hat(c)

            stage(t, USE_Q, 1, plan.q_chunks, q_use)


def store_kernel(plan, residual, q_mat, new_error, q_factor, sem, q_sem):
    def blocks(c):
        rows = pl.ds(pl.multiple_of(c * plan.p_rows, plan.p_rows), plan.p_rows)
        return pltpu.make_async_copy(residual.at[0, rows], new_error.at[0, rows], sem.at[c])

    last = pltpu.make_async_copy(q_mat, q_factor, q_sem)
    for c in range(plan.p_chunks):
        blocks(c).start()
    last.start()
    for c in range(plan.p_chunks):
        blocks(c).wait()
    last.wait()


def fused(plan, grad, error, q_init):
    rows, cols, rank = plan.rows, plan.cols, plan.rank
    pc, qc = plan.p_chunks, plan.q_chunks
    f32, bf16 = jnp.float32, jnp.bfloat16
    dma = pltpu.SemaphoreType.DMA
    dp, row, far = plan.n_dp - 1, plan.n_row - 1, plan.n_far - 1
    whole = pl.BlockSpec(memory_space=pltpu.VMEM)
    part = pltpu.VMEM((qc, plan.q_row, plan.q_cols), f32)
    residual, q_mat = pl.pallas_call(
        functools.partial(iterate_kernel, plan),
        out_shape=[pltpu.VMEM((1, rows, cols), bf16), pltpu.VMEM((cols, rank), f32)],
        in_specs=[pl.BlockSpec(memory_space=pl.ANY)] * 2 + [whole],
        out_specs=[whole] * 2,
        scratch_shapes=[
            pltpu.VMEM((rows, cols), bf16),
            pltpu.VMEM((cols, 2 * rank), bf16), pltpu.VMEM((2, rows, 2 * rank), bf16),
            pltpu.VMEM((2 * rank, rows), bf16),
            pltpu.VMEM((rows, rank), f32), pltpu.VMEM((rows, rank), f32),
            pltpu.VMEM((qc, rank, plan.q_cols), f32), pltpu.VMEM((qc, rank, plan.q_cols), f32),
            pltpu.VMEM((pc * plan.p_pair, rank), f32),
            pltpu.VMEM((far, pc * plan.p_far, rank), f32),
            pltpu.VMEM((dp, pc * plan.p_dp, rank), f32),
            pltpu.VMEM((row, qc, max(plan.q_row, plan.q_half), plan.q_cols), f32),
            part, part, part, part,
            pltpu.VMEM((qc, rank, plan.q_cols), f32),
            pltpu.VMEM((qc, plan.q_half, plan.q_cols), f32),
            pltpu.VMEM((rank, rank), f32), pltpu.VMEM((row, rank, rank), f32),
            pltpu.VMEM((rank, rank), f32), pltpu.VMEM((rank, rank), f32),
            dma((2, pc)), dma((2, row)), dma((2, pc)), dma((2, pc, far)),
            dma((2, pc, dp)), dma((2, pc, dp)), dma((2, pc, far)), dma((2, pc)),
            dma((2, qc, row)), dma((2, qc, row)), dma((2, qc)), dma((2, qc)),
            dma((2, qc)), dma((2, qc)), dma((2, qc)), dma((2, qc)), dma((2, qc)),
        ],
        compiler_params=pltpu.CompilerParams(
            collective_id=0, has_side_effects=True, vmem_limit_bytes=VMEM_BYTES
        ),
        name="iterate",
    )(grad, error, q_init)
    return pl.pallas_call(
        functools.partial(store_kernel, plan),
        out_shape=[
            jax.ShapeDtypeStruct((1, rows, cols), bf16), jax.ShapeDtypeStruct((cols, rank), f32)
        ],
        in_specs=[whole] * 2,
        out_specs=[pl.BlockSpec(memory_space=pl.ANY)] * 2,
        scratch_shapes=[dma((pc,)), dma(())],
        compiler_params=pltpu.CompilerParams(vmem_limit_bytes=4 << 20),
        name="store",
    )(residual, q_mat)


def solution(mesh):
    in_specs = (P("dp", "row", "col"), P("dp", "row", "col"), P("col", None))
    out_specs = (P("dp", "row", "col"), P("col", None))
    sizes = dict(mesh.shape)

    def step(grad, error, q_init):
        plan = Plan(sizes, grad.shape[1], grad.shape[2], q_init.shape[1])
        if plan.fits(sizes):
            return tuple(fused(plan, grad, error, q_init))
        return shards(grad, error, q_init)

    return jax.shard_map(step, mesh=mesh, in_specs=in_specs, out_specs=out_specs, check_vma=False)
```
